64 devices in a mesh: data: 4 (over x, y), tp: 16 (over z, core).
Axes of the slice: x: 2, y: 2, z: 8, core: 2. Of those that a mesh axis runs over, the one named last changes fastest.
The devices are a block of a 4x4x8 slice.
Arguments:
- hidden: bfloat16 [8, 1024, 2048], P('data'), parts along dimension 0
- seg_ids: int32 [8, 1024], P('data'), parts along dimension 0
- grad_out: bfloat16 [8, 1024, 2048], P('data'), parts along dimension 0
- gain_attn: float32 [2048], replicated
- gain_mlp: float32 [2048], replicated
- w_q: bfloat16 [2048, 2048], P(None, 'tp')
- w_k: bfloat16 [2048, 128], replicated
- w_v: bfloat16 [2048, 128], replicated
- w_o: bfloat16 [2048, 2048], P('tp')
- w_gate: bfloat16 [2048, 6656], P(None, 'tp')
- w_up: bfloat16 [2048, 6656], P(None, 'tp')
- w_down: bfloat16 [6656, 2048], P('tp')
Outputs:
- output 1: bfloat16 [8, 1024, 2048], P('data'), parts along dimension 0
- output 2: bfloat16 [8, 1024, 2048], P('data'), parts along dimension 0
- output 3: float32 [8192], P('data'), parts along dimension 0
- output 4: float32 [8192], P('data'), parts along dimension 0
- output 5: float32 [8192, 2048], P('data', 'tp'), parts along dimension 0
- output 6: float32 [8192, 128], P('data'), parts along dimension 0
- output 7: float32 [8192, 128], P('data'), parts along dimension 0
- output 8: float32 [8192, 2048], P(('data', 'tp')), parts along dimension 0
- output 9: float32 [8192, 6656], P('data', 'tp'), parts along dimension 0
- output 10: float32 [8192, 6656], P('data', 'tp'), parts along dimension 0
- output 11: float32 [26624, 2048], P(('data', 'tp')), parts along dimension 0
There are 4 independent parts. The reference program is written for one: setup_inputs(seed, part) draws one part's arguments, and reference() takes and returns one part's arrays. A program takes and returns all parts, laid end to end along the dimension named above; an argument that names none is the same for every part.
All inputs are finite; a program needn't handle non-finite values.
Results may differ from the reference program's by a relative error of at most 0.02.
Values are sent between devices in bfloat16 or wider.
A program may use at most 768 MiB of HBM per device.

```python
import jax
import jax.numpy as jnp
from jax import lax

D = 2048
FF = 6656
HEADS = 16
KV_HEADS = 1
HEAD = 128
SEQ = 1024
CUTS = 3
EPS = 1e-5


def draw_segments(key):
    cuts = jax.random.randint(key, (2, 1, CUTS), 1, SEQ)
    positions = jnp.arange(SEQ, dtype=jnp.int32)[None, :, None]
    return jnp.sum((positions >= cuts).astype(jnp.int32), axis=-1).astype(jnp.int32)


def draw_weight(key, n_rows, n_cols, scale):
    return (jax.random.normal(key, (n_rows, n_cols), jnp.float32) * scale).astype(jnp.bfloat16)


def setup_inputs(seed: int = 0, part: int = 0) -> dict:
    own_keys = jax.random.split(jax.random.fold_in(jax.random.key(seed), part), 3)
    shared = jax.random.split(jax.random.key(seed + 1), 9)
    qk_scale = 1.5 * D ** -0.5
    return {
        'hidden': jax.random.normal(own_keys[0], (2, SEQ, D), jnp.float32).astype(jnp.bfloat16),
        'seg_ids': draw_segments(own_keys[1]),
        'grad_out': jax.random.normal(own_keys[2], (2, SEQ, D), jnp.float32).astype(jnp.bfloat16),
        'gain_attn': 0.5 + jax.random.uniform(shared[0], (D,), jnp.float32),
        'gain_mlp': 0.5 + jax.random.uniform(shared[1], (D,), jnp.float32),
        'w_q': draw_weight(shared[2], D, HEADS * HEAD, qk_scale),
        'w_k': draw_weight(shared[3], D, KV_HEADS * HEAD, qk_scale),
        'w_v': draw_weight(shared[4], D, KV_HEADS * HEAD, D ** -0.5),
        'w_o': draw_weight(shared[5], HEADS * HEAD, D, (HEADS * HEAD) ** -0.5),
        'w_gate': draw_weight(shared[6], D, FF, D ** -0.5),
        'w_up': draw_weight(shared[7], D, FF, D ** -0.5),
        'w_down': draw_weight(shared[8], FF, D, FF ** -0.5),
    }


def rms_norm(x_in, gain):
    x_float = x_in.astype(jnp.float32)
    inv_rms = lax.rsqrt(jnp.mean(x_float * x_float, axis=-1, keepdims=True) + EPS)
    return (x_float * inv_rms * gain).astype(jnp.bfloat16)


def attention(q_all, k_all, v_all, seg_row):
    group = HEADS // KV_HEADS
    q_heads = q_all.reshape(SEQ, HEADS, HEAD).transpose(1, 0, 2)
    k_heads = jnp.repeat(k_all.reshape(SEQ, KV_HEADS, HEAD).transpose(1, 0, 2), group, axis=0)
    v_heads = jnp.repeat(v_all.reshape(SEQ, KV_HEADS, HEAD).transpose(1, 0, 2), group, axis=0)
    positions = jnp.arange(SEQ)
    allowed = (positions[:, None] >= positions[None, :]) & (seg_row[:, None] == seg_row[None, :])

    def one_head(operands):
        q_head, k_head, v_head = operands
        scores = jnp.dot(q_head.astype(jnp.float32), k_head.astype(jnp.float32).T) * HEAD ** -0.5
        scores = jnp.where(allowed, scores, -1e30)
        probs = jax.nn.softmax(scores, axis=-1).astype(jnp.bfloat16)
        return jnp.dot(probs, v_head, preferred_element_type=jnp.float32)

    ctx = lax.map(jax.checkpoint(one_head), (q_heads, k_heads, v_heads))
    return ctx.transpose(1, 0, 2).reshape(SEQ, HEADS * HEAD).astype(jnp.bfloat16)


def layer(x_half, seg_row, gain_attn, gain_mlp, w_q, w_k, w_v, w_o, w_gate, w_up, w_down):
    normed = rms_norm(x_half, gain_attn)
    q_all = jnp.dot(normed, w_q, preferred_element_type=jnp.float32).astype(jnp.bfloat16)
    k_all = jnp.dot(normed, w_k, preferred_element_type=jnp.float32).astype(jnp.bfloat16)
    v_all = jnp.dot(normed, w_v, preferred_element_type=jnp.float32).astype(jnp.bfloat16)
    ctx = attention(q_all, k_all, v_all, seg_row)
    attn_out = jnp.dot(ctx, w_o, preferred_element_type=jnp.float32).astype(jnp.bfloat16)
    resid = (x_half.astype(jnp.float32) + attn_out.astype(jnp.float32)).astype(jnp.bfloat16)
    mixed = rms_norm(resid, gain_mlp)
    gate = jnp.dot(mixed, w_gate, preferred_element_type=jnp.float32)
    upper = jnp.dot(mixed, w_up, preferred_element_type=jnp.float32)
    act = (jax.nn.silu(gate) * upper).astype(jnp.bfloat16)
    mlp_out = jnp.dot(act, w_down, preferred_element_type=jnp.float32).astype(jnp.bfloat16)
    return (resid.astype(jnp.float32) + mlp_out.astype(jnp.float32)).astype(jnp.bfloat16)


def reference(hidden, seg_ids, grad_out, gain_attn, gain_mlp, w_q, w_k, w_v, w_o, w_gate, w_up, w_down):
    params = (gain_attn, gain_mlp, w_q, w_k, w_v, w_o, w_gate, w_up, w_down)
    y_halves = []
    dx_halves = []
    totals = [jnp.zeros(param.shape, jnp.float32) for param in params]
    for half_idx in range(2):
        seg_row = seg_ids[half_idx]

        def half_layer(x_half, *weights):
            return layer(x_half, seg_row, *weights)

        y_half, pullback = jax.vjp(half_layer, hidden[half_idx], *params)
        cotangents = pullback(grad_out[half_idx])
        y_halves.append(y_half)
        dx_halves.append(cotangents[0])
        totals = [acc_val + cot_val.astype(jnp.float32) for acc_val, cot_val in zip(totals, cotangents[1:])]
    return (jnp.stack(y_halves), jnp.stack(dx_halves), totals[0], totals[1], totals[2], totals[3], totals[4], totals[5], totals[6], totals[7], totals[8])
```

```python
import functools
import jax
import jax.numpy as jnp
from jax import lax
from jax.experimental import pallas as pl
from jax.experimental.pallas import tpu as pltpu
from jax.sharding import PartitionSpec as P

HEAD_DIM = 128
EPS = 1e-5
SUB = 4
ROWS = 16
BLK = 256
BF = jnp.bfloat16
F32 = jnp.float32
MESH = pl.DeviceIdType.MESH
VMEM_LIMIT = 60 * 1024 * 1024


def mm(a, b):
    return lax.dot_general(a, b, (((1,), (0,)), ((), ())), preferred_element_type=F32)


def mm_nt(a, b):
    return lax.dot_general(a, b, (((1,), (1,)), ((), ())), preferred_element_type=F32)


def mm_tn(a, b):
    return lax.dot_general(a, b, (((0,), (0,)), ((), ())), preferred_element_type=F32)


def rms_parts(x_in):
    x_float = x_in.astype(F32)
    inv = lax.rsqrt(jnp.mean(x_float * x_float, axis=-1, keepdims=True) + EPS)
    return x_float * inv, inv


def rms_back(grad, normed, inv, gain):
    scaled = grad * gain
    return inv * (scaled - normed * jnp.mean(scaled * normed, axis=-1, keepdims=True))


def ring_kernel(chips, n_in, n_out, epilogue, with_gain, part, *refs):
    ins = refs[:n_in]
    out = refs[n_in]
    outs = refs[n_in + 1:n_in + 1 + n_out]
    scratch = refs[n_in + 1 + n_out:]
    (loc, oth, arr, gat, ld_sem, xs_sem, xr_sem, rs_sem, rr_sem, as_sem, ar_sem, ps_sem, pr_sem, wo_sem) = scratch[:14]
    me = lax.axis_index('tp')
    chip = me // 2
    core = me % 2
    mate = chip * 2 + 1 - core
    nxt = (lax.rem(chip + 1, chips) * 2 + core, lax.rem(chip + chips - 1, chips) * 2 + core)

    def dev(t):
        return {'tp': t}

    barrier = pltpu.get_barrier_semaphore()
    for t in (nxt[0], nxt[1], mate):
        pl.semaphore_signal(barrier, inc=1, device_id=dev(t), device_id_type=MESH)
    pl.semaphore_wait(barrier, 3)

    def chunk_at(d, s):
        off = s if d == 1 else chips - s
        return lax.rem(chip + off, chips)

    def swap(d, s):
        m = chunk_at(d, s)
        return pltpu.make_async_remote_copy(
            src_ref=part.at[m * 2 + 1 - core, d], dst_ref=oth.at[m, d], send_sem=xs_sem,
            recv_sem=xr_sem.at[m, d], device_id=dev(mate), device_id_type=MESH)

    def load(d, s):
        m = chunk_at(d, s)
        return pltpu.make_async_copy(part.at[m * 2 + core, d], loc.at[m, d], ld_sem.at[m, d])

    if with_gain:
        (gacc, gbuf, gmate, gs_sem, gr_sem, gms_sem, gmr_sem, kacc, koth, karr, kxs, kxr, krs, krr, kas, kar, kps, kpr) = scratch[14:]
        kin, kout = ins[5], outs[1]

        def kswap(d, s):
            m = chunk_at(d, s)
            return pltpu.make_async_remote_copy(
                src_ref=kin.at[m * 2 + 1 - core, d], dst_ref=koth.at[m, d], send_sem=kxs,
                recv_sem=kxr.at[m, d], device_id=dev(mate), device_id_type=MESH)

        def krs_copy(d, s, m):
            return pltpu.make_async_remote_copy(
                src_ref=kacc.at[m, d], dst_ref=karr.at[s, d], send_sem=krs,
                recv_sem=krr.at[s, d], device_id=dev(nxt[d]), device_id_type=MESH)

        def kag_copy(d, t, m):
            return pltpu.make_async_remote_copy(
                src_ref=kout.at[m * 2 + core, d], dst_ref=kout.at[m * 2 + core, d], send_sem=kas,
                recv_sem=kar.at[t, d], device_id=dev(nxt[d]), device_id_type=MESH)

        def kspread(d, m):
            pltpu.make_async_remote_copy(
                src_ref=kout.at[m * 2 + core, d], dst_ref=kout.at[m * 2 + core, d], send_sem=kps,
                recv_sem=kpr, device_id=dev(mate), device_id_type=MESH).start()

    for s in range(1, chips + 1):
        for d in range(2):
            swap(d, s % chips).start()
            load(d, s % chips).start()
            if with_gain:
                kswap(d, s % chips).start()

    def rs_copy(d, j, s, m):
        return pltpu.make_async_remote_copy(
            src_ref=loc.at[m, d, j], dst_ref=arr.at[s, d, j], send_sem=rs_sem,
            recv_sem=rr_sem.at[s, d, j], device_id=dev(nxt[d]), device_id_type=MESH)

    def ready(d, s):
        load(d, s).wait()
        swap(d, s).wait_recv()

    def rs_step(s, first):
        for d in range(2):
            ready(d, s + 1)
        for j in range(SUB):
            for d in range(2):
                m = chunk_at(d, s + 1)
                v = loc[m, d, j].astype(F32) + oth[m, d, j].astype(F32)
                if not first:
                    rs_copy(d, j, s - 1, m).wait_recv()
                    v = v + arr[s - 1, d, j].astype(F32)
                loc[m, d, j] = v.astype(BF)
                rs_copy(d, j, s, m).start()
        if with_gain:
            for d in range(2):
                m = chunk_at(d, s + 1)
                kswap(d, s + 1).wait_recv()
                kv = kin[m * 2 + core, d] + koth[m, d]
                if not first:
                    krs_copy(d, s - 1, m).wait_recv()
                    kv = kv + karr[s - 1, d]
                kacc[m, d] = kv
                krs_copy(d, s, m).start()

    rs_step(0, True)

    @pl.loop(1, chips - 1)
    def _(s):
        rs_step(s, False)

    def ag_copy(d, j, t, m):
        return pltpu.make_async_remote_copy(
            src_ref=gat.at[m, d, j], dst_ref=gat.at[m, d, j], send_sem=as_sem,
            recv_sem=ar_sem.at[t, d, j], device_id=dev(nxt[d]), device_id_type=MESH)

    def spread(d, j, m):
        pltpu.make_async_remote_copy(
            src_ref=gat.at[m, d, j], dst_ref=out.at[m * 2 + core, d, j], send_sem=ps_sem,
            recv_sem=pr_sem, device_id=dev(mate), device_id_type=MESH).start()
        pltpu.make_async_copy(gat.at[m, d, j], out.at[m * 2 + core, d, j], wo_sem).start()

    for d in range(2):
        ready(d, 0)
    state = epilogue.begin(ins, outs)
    for j in range(SUB):
        for d in range(2):
            rs_copy(d, j, chips - 2, chip).wait_recv()
            v = loc[chip, d, j].astype(F32) + oth[chip, d, j].astype(F32) + arr[chips - 2, d, j].astype(F32)
            res, state = epilogue.piece(v.astype(BF).astype(F32), d, j, ins, outs, state)
            gat[chip, d, j] = res
            ag_copy(d, j, 0, chip).start()
            spread(d, j, chip)
    epilogue.end(outs, state)

    if with_gain:
        for d in range(2):
            kswap(d, 0).wait_recv()
            krs_copy(d, chips - 2, chip).wait_recv()
            kout[chip * 2 + core, d] = kin[chip * 2 + core, d] + koth[chip, d] + karr[chips - 2, d]
            kag_copy(d, 0, chip).start()
            kspread(d, chip)

        def gain_copy(t, src):
            return pltpu.make_async_remote_copy(
                src_ref=src, dst_ref=gbuf.at[t], send_sem=gs_sem.at[t],
                recv_sem=gr_sem.at[t], device_id=dev(nxt[0]), device_id_type=MESH)

        gacc[0:1] = ins[4][...]
        gacc[1:2] = state
        gain_copy(0, gacc).start()

    def ag_step(t, last):
        for j in range(SUB):
            for d in range(2):
                m = chunk_at(d, t)
                ag_copy(d, j, t - 1, m).wait_recv()
                if not last:
                    ag_copy(d, j, t, m).start()
                spread(d, j, m)
        if with_gain:
            for d in range(2):
                m = chunk_at(d, t)
                kag_copy(d, t - 1, m).wait_recv()
                if not last:
                    kag_copy(d, t, m).start()
                kspread(d, m)
            gain_copy(t - 1, gacc).wait_recv()
            if not last:
                gain_copy(t, gbuf.at[t - 1]).start()

    @pl.loop(1, chips - 1)
    def _(t):
        ag_step(t, False)

    ag_step(chips - 1, True)

    if with_gain:
        tot = gacc[...]
        for t in range(chips - 1):
            tot = tot + gbuf[t]
            gain_copy(t, gacc).wait_send()
        outs[0][...] = tot
        mate_copy = pltpu.make_async_remote_copy(
            src_ref=outs[0], dst_ref=gmate, send_sem=gms_sem, recv_sem=gmr_sem,
            device_id=dev(mate), device_id_type=MESH)
        mate_copy.start()
        mate_copy.wait()
        outs[0][...] = tot + gmate[...]

    def bulk(ref, sem, rsem):
        return pltpu.make_async_remote_copy(
            src_ref=ref, dst_ref=ref, send_sem=sem, recv_sem=rsem, device_id=dev(mate), device_id_type=MESH)

    if with_gain:
        bulk(koth, kps, kpr).wait_recv()
        bulk(koth, kxs, kpr).wait_send()
        bulk(karr, krs, kpr).wait_send()
        bulk(karr, kas, kpr).wait_send()
        bulk(koth, kps, kpr).wait_send()
    bulk(gat, ps_sem, pr_sem).wait_recv()
    bulk(oth, xs_sem, pr_sem).wait_send()
    bulk(arr, rs_sem, pr_sem).wait_send()
    bulk(arr, as_sem, pr_sem).wait_send()
    bulk(gat, ps_sem, pr_sem).wait_send()
    pltpu.make_async_copy(gat, gat, wo_sem).wait()


class ForwardTail:
    @staticmethod
    def begin(ins, outs):
        return None

    @staticmethod
    def piece(v, d, j, ins, outs, state):
        h = (ins[0][d, j].astype(F32) + v).astype(BF)
        outs[0][d, j] = h
        normed, _ = rms_parts(h)
        return (normed * ins[1][...]).astype(BF), state

    @staticmethod
    def end(outs, state):
        pass


class AddTail:
    @staticmethod
    def begin(ins, outs):
        return None

    @staticmethod
    def piece(v, d, j, ins, outs, state):
        return (ins[0][d, j].astype(F32) + v).astype(BF), state

    @staticmethod
    def end(outs, state):
        pass


class MlpTail:
    @staticmethod
    def begin(ins, outs):
        return jnp.zeros(ins[2].shape, F32)

    @staticmethod
    def piece(v, d, j, ins, outs, state):
        normed, inv = rms_parts(ins[0][d, j])
        state = state + jnp.sum(v * normed, axis=0, keepdims=True)
        grad = ins[1][d, j].astype(F32) + rms_back(v, normed, inv, ins[2][...])
        outs[0][d, j] = grad
        return grad.astype(BF), state

    @staticmethod
    def end(outs, state):
        outs[1][...] = state


class AttnTail:
    @staticmethod
    def begin(ins, outs):
        return jnp.zeros(ins[2].shape, F32)

    @staticmethod
    def piece(v, d, j, ins, outs, state):
        normed, inv = rms_parts(ins[0][d, j])
        state = state + jnp.sum(v * normed, axis=0, keepdims=True)
        grad = ins[1][d, j] + rms_back(v, normed, inv, ins[2][...])
        return grad.astype(BF), state

    @staticmethod
    def end(outs, state):
        pass


def ring_call(part, ins, out_shapes, epilogue, chips, cid, with_gain=False):
    tokens, width = part.shape
    shape = (chips * 2, 2, SUB, ROWS, width)
    half = (chips, 2, SUB, ROWS, width)
    arrive = (chips - 1, 2, SUB, ROWS, width)
    vm = pl.BlockSpec(memory_space=pltpu.VMEM)
    anyspec = pl.BlockSpec(memory_space=pl.ANY)
    dma = pltpu.SemaphoreType.DMA
    scratch = [
        pltpu.VMEM(half, BF), pltpu.VMEM(half, BF), pltpu.VMEM(arrive, BF), pltpu.VMEM(half, BF),
        dma((chips, 2)), dma, dma((chips, 2)), dma, dma((chips - 1, 2, SUB)), dma,
        dma((chips - 1, 2, SUB)), dma, dma, dma]
    if with_gain:
        scratch += [pltpu.VMEM((2, width), F32), pltpu.VMEM((chips - 1, 2, width), F32), pltpu.VMEM((2, width), F32),
                    dma((chips - 1,)), dma((chips - 1,)), dma, dma]
        kshape = ins[5].shape[1:]
        scratch += [pltpu.VMEM((chips,) + kshape, F32), pltpu.VMEM((chips,) + kshape, F32), pltpu.VMEM((chips - 1,) + kshape, F32),
                    dma, dma((chips, 2)), dma, dma((chips - 1, 2)), dma, dma((chips - 1, 2)), dma, dma]
    n_in, n_out = len(ins), len(out_shapes)

    def body(*refs):
        ring_kernel(chips, n_in, n_out, epilogue, with_gain, *refs)

    res = pl.pallas_call(
        body,
        out_shape=[jax.ShapeDtypeStruct(shape, BF)] + out_shapes,
        in_specs=[anyspec] + [vm] * n_in,
        out_specs=[anyspec] + [vm] * n_out,
        scratch_shapes=scratch,
        name='ring_%d' % cid,
        compiler_params=pltpu.CompilerParams(collective_id=cid, has_side_effects=True, vmem_limit_bytes=VMEM_LIMIT),
        cost_estimate=pl.CostEstimate(flops=80_000_000_000, bytes_accessed=4 * tokens * width, transcendentals=0),
    )(part.reshape(shape), *ins)
    return (res[0].reshape(tokens, width),) + tuple(res[1:])


def masked_probs(q, k, seg_ref, b, row0):
    n = q.shape[0]
    seg_k = seg_ref[pl.ds(b, 1), :].astype(F32)
    own = seg_ref[pl.ds(b, 1), pl.ds(row0, n)].astype(F32)
    seg_q = jnp.transpose(jnp.broadcast_to(own, (128, n)))[:, :1]
    s = mm_nt(q, k) * HEAD_DIM ** -0.5
    rows = row0 + lax.broadcasted_iota(jnp.int32, s.shape, 0)
    cols = lax.broadcasted_iota(jnp.int32, s.shape, 1)
    s = jnp.where((rows >= cols) & (seg_q == seg_k), s, -1e30)
    e = jnp.exp(s - jnp.max(s, axis=-1, keepdims=True))
    return e * (1.0 / jnp.sum(e, axis=-1, keepdims=True))


def pack(w_ref, wq_ref, wk_ref, wv_ref):
    for n, ref in enumerate((wq_ref, wk_ref, wv_ref)):
        w_ref[:, n * HEAD_DIM:(n + 1) * HEAD_DIM] = ref[...]


def front_kernel(x_ref, sg_ref, g_ref, wq_ref, wk_ref, wv_ref, wo_ref, o_ref, qkv_ref, ctx_ref, k_s, v_s, w_ref):
    qi = pl.program_id(1)

    @pl.when((qi == 0) & (pl.program_id(0) == 0))
    def _():
        k_s[...] = jnp.zeros_like(k_s)
        v_s[...] = jnp.zeros_like(v_s)
        pack(w_ref, wq_ref, wk_ref, wv_ref)

    normed, _ = rms_parts(x_ref[0])
    a = (normed * g_ref[...]).astype(BF)
    qkv = mm(a, w_ref[...]).astype(BF)
    qkv_ref[0] = qkv
    row0 = pl.multiple_of(qi * BLK, BLK)
    k_s[pl.ds(row0, BLK)] = qkv[:, HEAD_DIM:2 * HEAD_DIM]
    v_s[pl.ds(row0, BLK)] = qkv[:, 2 * HEAD_DIM:]
    probs = masked_probs(qkv[:, :HEAD_DIM], k_s[...], sg_ref, pl.program_id(0), row0)
    ctx = mm(probs.astype(BF), v_s[...]).astype(BF)
    ctx_ref[0] = ctx
    o_ref[0] = mm(ctx, wo_ref[...]).astype(BF)


def front_call(x, seg, gain, w_q, w_k, w_v, w_o):
    nb, seq, width = x.shape
    e3 = 3 * HEAD_DIM
    rowblk = lambda n: pl.BlockSpec((1, BLK, n), lambda b, i: (b, i, 0))
    whole = lambda arr: pl.BlockSpec(arr.shape, lambda b, i: (0, 0))
    return pl.pallas_call(
        front_kernel,
        grid=(nb, seq // BLK),
        in_specs=[rowblk(width), whole(seg), whole(gain), whole(w_q), whole(w_k), whole(w_v), whole(w_o)],
        out_specs=[rowblk(width), rowblk(e3), rowblk(HEAD_DIM)],
        out_shape=[jax.ShapeDtypeStruct((nb, seq, width), BF), jax.ShapeDtypeStruct((nb, seq, e3), BF),
                   jax.ShapeDtypeStruct((nb, seq, HEAD_DIM), BF)],
        scratch_shapes=[pltpu.VMEM((seq, HEAD_DIM), BF), pltpu.VMEM((seq, HEAD_DIM), BF), pltpu.VMEM((width, e3), BF)],
        name='front',
        compiler_params=pltpu.CompilerParams(vmem_limit_bytes=VMEM_LIMIT),
        cost_estimate=pl.CostEstimate(flops=8_000_000_000, bytes_accessed=20_000_000, transcendentals=0),
    )(x, seg, gain, w_q, w_k, w_v, w_o)


def back_kernel(dr_ref, x_ref, sg_ref, g_ref, wq_ref, wk_ref, wv_ref, wo_ref, q_ref, qkv_ref, ctx_ref,
                ga_ref, dwq_ref, dkv_ref, dwo_ref, dqkv_s, dk_s, dv_s, w_ref):
    b, ph = pl.program_id(0), pl.program_id(1)
    nq = pl.num_programs(1) // 2
    scale = HEAD_DIM ** -0.5

    @pl.when((ph == 0) & (b == 0))
    def _():
        pack(w_ref, wq_ref, wk_ref, wv_ref)
        dwq_ref[...] = jnp.zeros_like(dwq_ref)
        dkv_ref[...] = jnp.zeros_like(dkv_ref)
        dwo_ref[...] = jnp.zeros_like(dwo_ref)

    @pl.when(ph == 0)
    def _():
        dk_s[...] = jnp.zeros_like(dk_s)
        dv_s[...] = jnp.zeros_like(dv_s)

    @pl.when(ph < nq)
    def _():
        row0 = pl.multiple_of(ph * BLK, BLK)
        dr = dr_ref[0]
        dctx = mm_nt(dr, wo_ref[...]).astype(BF)
        dwo_ref[...] += mm_tn(ctx_ref[0], dr)
        q = q_ref[0]
        k = qkv_ref[0, :, HEAD_DIM:2 * HEAD_DIM]
        v = qkv_ref[0, :, 2 * HEAD_DIM:]
        probs = masked_probs(q, k, sg_ref, b, row0)
        dp = mm_nt(dctx, v)
        ds = (probs * (dp - jnp.sum(dp * probs, axis=-1, keepdims=True)) * scale).astype(BF)
        dv_s[...] += mm_tn(probs.astype(BF), dctx)
        dk_s[...] += mm_tn(ds, q)
        dqkv_s[pl.ds(row0, BLK), :HEAD_DIM] = mm(ds, k).astype(BF)

    @pl.when(ph == nq - 1)
    def _():
        dqkv_s[:, HEAD_DIM:2 * HEAD_DIM] = dk_s[...].astype(BF)
        dqkv_s[:, 2 * HEAD_DIM:] = dv_s[...].astype(BF)

    @pl.when(ph >= nq)
    def _():
        row0 = pl.multiple_of((ph - nq) * BLK, BLK)
        normed, _ = rms_parts(x_ref[0])
        a = (normed * g_ref[...]).astype(BF)
        blk = dqkv_s[pl.ds(row0, BLK)]
        dw = mm_tn(a, blk)
        dwq_ref[...] += dw[:, :HEAD_DIM]
        dkv_ref[...] += dw[:, HEAD_DIM:]
        ga_ref[0] = mm_nt(blk, w_ref[...]).astype(BF)


def back_call(dr, x, seg, gain, w_q, w_k, w_v, w_o, qkv, ctx):
    nb, seq, width = x.shape
    nq = seq // BLK
    e3 = 3 * HEAD_DIM
    first = lambda n: pl.BlockSpec((1, BLK, n), lambda b, i: (b, jnp.minimum(i, nq - 1), 0))
    second = lambda n: pl.BlockSpec((1, BLK, n), lambda b, i: (b, jnp.maximum(i - nq, 0), 0))
    whole = lambda arr: pl.BlockSpec(arr.shape, lambda b, i: (0, 0))
    const = lambda shp: pl.BlockSpec(shp, lambda b, i: (0, 0))
    return pl.pallas_call(
        back_kernel,
        grid=(nb, 2 * nq),
        in_specs=[first(width), second(width), whole(seg), whole(gain), whole(w_q), whole(w_k), whole(w_v), whole(w_o),
                  first(HEAD_DIM), pl.BlockSpec((1, seq, e3), lambda b, i: (b, 0, 0)), first(HEAD_DIM)],
        out_specs=[second(width), const((width, HEAD_DIM)), const((width, 2 * HEAD_DIM)), const((HEAD_DIM, width))],
        out_shape=[jax.ShapeDtypeStruct((nb, seq, width), BF), jax.ShapeDtypeStruct((width, HEAD_DIM), F32),
                   jax.ShapeDtypeStruct((width, 2 * HEAD_DIM), F32),
                   jax.ShapeDtypeStruct((HEAD_DIM, width), F32)],
        scratch_shapes=[pltpu.VMEM((seq, e3), BF), pltpu.VMEM((seq, HEAD_DIM), F32), pltpu.VMEM((seq, HEAD_DIM), F32), pltpu.VMEM((width, e3), BF)],
        name='back',
        compiler_params=pltpu.CompilerParams(vmem_limit_bytes=VMEM_LIMIT),
        cost_estimate=pl.CostEstimate(flops=12_000_000_000, bytes_accessed=30_000_000, transcendentals=0),
    )(dr, x, seg, gain, w_q, w_k, w_v, w_o, qkv, qkv, ctx)


def mlp_kernel(m_ref, dy_ref, wg_ref, wu_ref, wd_ref, p_ref, gm_ref, dwg_ref, dwu_ref, dwd_ref):
    @pl.when(pl.program_id(0) == 0)
    def _():
        dwg_ref[...] = jnp.zeros_like(dwg_ref)
        dwu_ref[...] = jnp.zeros_like(dwu_ref)
        dwd_ref[...] = jnp.zeros_like(dwd_ref)

    m = m_ref[...]
    dy = dy_ref[...]
    gate = mm_nt(m, wg_ref[...])
    upper = mm_nt(m, wu_ref[...])
    sig = jax.nn.sigmoid(gate)
    act = (gate * sig * upper).astype(BF)
    p_ref[...] = mm(act, wd_ref[...]).astype(BF)
    dact = mm_nt(dy, wd_ref[...])
    dwd_ref[...] += mm_tn(act, dy)
    dgate = (dact * upper * sig * (1.0 + gate * (1.0 - sig))).astype(BF)
    dupper = (dact * gate * sig).astype(BF)
    dwg_ref[...] += mm_tn(dgate, m)
    dwu_ref[...] += mm_tn(dupper, m)
    gm_ref[...] = (mm(dgate, wg_ref[...]) + mm(dupper, wu_ref[...])).astype(BF)


def mlp_call(m, dy, w_gate, w_up, w_down):
    tokens, width = m.shape
    ff = w_down.shape[0]
    rowblk = pl.BlockSpec((BLK, width), lambda i: (i, 0))
    const = lambda shp: pl.BlockSpec(shp, lambda i: (0, 0))
    return pl.pallas_call(
        mlp_kernel,
        grid=(tokens // BLK,),
        in_specs=[rowblk, rowblk, const((ff, width)), const((ff, width)), const((ff, width))],
        out_specs=[rowblk, rowblk, const((ff, width)), const((ff, width)), const((ff, width))],
        out_shape=[jax.ShapeDtypeStruct((tokens, width), BF), jax.ShapeDtypeStruct((tokens, width), BF),
                   jax.ShapeDtypeStruct((ff, width), F32), jax.ShapeDtypeStruct((ff, width), F32),
                   jax.ShapeDtypeStruct((ff, width), F32)],
        name='mlp',
        compiler_params=pltpu.CompilerParams(vmem_limit_bytes=VMEM_LIMIT),
        cost_estimate=pl.CostEstimate(flops=32_000_000_000, bytes_accessed=50_000_000, transcendentals=0),
    )(m, dy, w_gate, w_up, w_down)


def solution(mesh):
    tp_size = mesh.shape['tp']
    chips = tp_size // 2

    def device_step(hidden, seg_ids, grad_out, gain_attn, gain_mlp, w_q, w_k, w_v, w_o, w_gate, w_up, w_down):
        nb, seq, width = hidden.shape
        tokens = nb * seq
        own = tokens // tp_size
        row0 = lax.axis_index('tp') * own
        piece = (2, SUB, ROWS, width)

        def own_rows(arr):
            return lax.dynamic_slice_in_dim(arr.reshape(tokens, width), row0, own, axis=0).reshape(piece)

        g1 = gain_attn[None, :]
        g2 = gain_mlp[None, :]
        x_own = own_rows(hidden)
        dy_own = own_rows(grad_out)
        shard_bf = jax.ShapeDtypeStruct(piece, BF)
        shard_f = jax.ShapeDtypeStruct(piece, F32)
        gain_f = jax.ShapeDtypeStruct((1, width), F32)
        weights = (w_q, w_k, w_v, w_o)

        o_part, qkv, ctx = front_call(hidden, seg_ids, g1, *weights)
        mixed, h_own = ring_call(o_part.reshape(tokens, width), [x_own, g2], [shard_bf], ForwardTail, chips, 1)
        p_part, gm_part, d_gate, d_up, d_down = mlp_call(mixed, grad_out.reshape(tokens, width), w_gate.T, w_up.T, w_down)
        dres, dres_own, g2_part = ring_call(gm_part, [h_own, dy_own, g2], [shard_f, gain_f], MlpTail, chips, 2)
        ga_part, d_q, d_kv, d_o = back_call(dres.reshape(nb, seq, width), hidden, seg_ids, g1, *weights, qkv, ctx)
        (y_out,) = ring_call(p_part, [h_own], [], AddTail, chips, 4)
        kv_rows = own // 2
        kv_shape = (tp_size, 2, kv_rows, 2 * HEAD_DIM)
        dx, gains, d_kv = ring_call(ga_part.reshape(tokens, width), [x_own, dres_own, g1, g1, g2_part, d_kv.reshape(kv_shape)],
                                    [jax.ShapeDtypeStruct((2, width), F32), jax.ShapeDtypeStruct(kv_shape, F32)], AttnTail, chips, 3, True)
        d_kv = d_kv.reshape(width, 2 * HEAD_DIM)
        return (y_out.reshape(nb, seq, width), dx.reshape(nb, seq, width), gains[1], gains[0], d_q, d_kv[:, :HEAD_DIM], d_kv[:, HEAD_DIM:],
                d_o, d_gate.T, d_up.T, d_down)

    spec_act = P('data', None, None)
    spec_rows = P('data', None)
    spec_gain = P(None)
    spec_cols = P(None, 'tp')
    spec_tprows = P('tp', None)
    spec_whole = P(None, None)
    spec_stack = P(('data', 'tp'), None)
    in_specs = (spec_act, spec_rows, spec_act, spec_gain, spec_gain, spec_cols, spec_whole, spec_whole, spec_tprows, spec_cols, spec_cols, spec_tprows)
    out_specs = (spec_act, spec_act, P('data'), P('data'), P('data', 'tp'), spec_rows, spec_rows, spec_stack, P('data', 'tp'), P('data', 'tp'), spec_stack)
    return jax.shard_map(device_step, mesh=mesh, in_specs=in_specs, out_specs=out_specs, check_vma=False)
```

```python
import functools
import jax
import jax.numpy as jnp
from jax import lax
from jax.experimental import pallas as pl
from jax.experimental.pallas import tpu as pltpu
from jax.sharding import PartitionSpec as P

HEAD_DIM = 128
EPS = 1e-5
SUB = 4
ROWS = 16
BLK = 256
BF = jnp.bfloat16
F32 = jnp.float32
MESH = pl.DeviceIdType.MESH
VMEM_LIMIT = 60 * 1024 * 1024


def mm(a, b):
    return lax.dot_general(a, b, (((1,), (0,)), ((), ())), preferred_element_type=F32)


def mm_nt(a, b):
    return lax.dot_general(a, b, (((1,), (1,)), ((), ())), preferred_element_type=F32)


def mm_tn(a, b):
    return lax.dot_general(a, b, (((0,), (0,)), ((), ())), preferred_element_type=F32)


def rms_parts(x_in):
    x_float = x_in.astype(F32)
    inv = lax.rsqrt(jnp.mean(x_float * x_float, axis=-1, keepdims=True) + EPS)
    return x_float * inv, inv


def rms_back(grad, normed, inv, gain):
    scaled = grad * gain
    return inv * (scaled - normed * jnp.mean(scaled * normed, axis=-1, keepdims=True))


def ring_kernel(chips, n_in, n_out, epilogue, with_gain, part, *refs):
    ins = refs[:n_in]
    out = refs[n_in]
    outs = refs[n_in + 1:n_in + 1 + n_out]
    scratch = refs[n_in + 1 + n_out:]
    (loc, oth, arr, gat, ld_sem, xs_sem, xr_sem, rs_sem, rr_sem, as_sem, ar_sem, ps_sem, pr_sem, wo_sem) = scratch[:14]
    me = lax.axis_index('tp')
    chip = me // 2
    core = me % 2
    mate = chip * 2 + 1 - core
    nxt = (lax.rem(chip + 1, chips) * 2 + core, lax.rem(chip + chips - 1, chips) * 2 + core)

    def dev(t):
        return {'tp': t}

    barrier = pltpu.get_barrier_semaphore()
    for t in (nxt[0], nxt[1], mate):
        pl.semaphore_signal(barrier, inc=1, device_id=dev(t), device_id_type=MESH)
    pl.semaphore_wait(barrier, 3)

    def chunk_at(d, s):
        off = s if d == 1 else chips - s
        return lax.rem(chip + off, chips)

    def swap(d, s):
        m = chunk_at(d, s)
        return pltpu.make_async_remote_copy(
            src_ref=part.at[m * 2 + 1 - core, d], dst_ref=oth.at[m, d], send_sem=xs_sem,
            recv_sem=xr_sem.at[m, d], device_id=dev(mate), device_id_type=MESH)

    def load(d, s):
        m = chunk_at(d, s)
        return pltpu.make_async_copy(part.at[m * 2 + core, d], loc.at[m, d], ld_sem.at[m, d])

    if with_gain:
        (gacc, gbuf, gmate, gs_sem, gr_sem, gms_sem, gmr_sem, kacc, koth, karr, kxs, kxr, krs, krr, kas, kar, kps, kpr) = scratch[14:]
        kin, kout = ins[5], outs[1]

        def kswap(d, s):
            m = chunk_at(d, s)
            return pltpu.make_async_remote_copy(
                src_ref=kin.at[m * 2 + 1 - core, d], dst_ref=koth.at[m, d], send_sem=kxs,
                recv_sem=kxr.at[m, d], device_id=dev(mate), device_id_type=MESH)

        def krs_copy(d, s, m):
            return pltpu.make_async_remote_copy(
                src_ref=kacc.at[m, d], dst_ref=karr.at[s, d], send_sem=krs,
                recv_sem=krr.at[s, d], device_id=dev(nxt[d]), device_id_type=MESH)

        def kag_copy(d, t, m):
            return pltpu.make_async_remote_copy(
                src_ref=kout.at[m * 2 + core, d], dst_ref=kout.at[m * 2 + core, d], send_sem=kas,
                recv_sem=kar.at[t, d], device_id=dev(nxt[d]), device_id_type=MESH)

        def kspread(d, m):
            pltpu.make_async_remote_copy(
                src_ref=kout.at[m * 2 + core, d], dst_ref=kout.at[m * 2 + core, d], send_sem=kps,
                recv_sem=kpr, device_id=dev(mate), device_id_type=MESH).start()

    for s in range(1, chips + 1):
        for d in range(2):
            swap(d, s % chips).start()
            load(d, s % chips).start()
            if with_gain:
                kswap(d, s % chips).start()

    def rs_copy(d, j, s, m):
        return pltpu.make_async_remote_copy(
            src_ref=loc.at[m, d, j], dst_ref=arr.at[s, d, j], send_sem=rs_sem,
            recv_sem=rr_sem.at[s, d, j], device_id=dev(nxt[d]), device_id_type=MESH)

    def ready(d, s):
        load(d, s).wait()
        swap(d, s).wait_recv()

    def rs_step(s, first):
        for d in range(2):
            ready(d, s + 1)
        for j in range(SUB):
            for d in range(2):
                m = chunk_at(d, s + 1)
                v = loc[m, d, j].astype(F32) + oth[m, d, j].astype(F32)
                if not first:
                    rs_copy(d, j, s - 1, m).wait_recv()
                    v = v + arr[s - 1, d, j].astype(F32)
                loc[m, d, j] = v.astype(BF)
                rs_copy(d, j, s, m).start()
        if with_gain:
            for d in range(2):
                m = chunk_at(d, s + 1)
                kswap(d, s + 1).wait_recv()
                kv = kin[m * 2 + core, d] + koth[m, d]
                if not first:
                    krs_copy(d, s - 1, m).wait_recv()
                    kv = kv + karr[s - 1, d]
                kacc[m, d] = kv
                krs_copy(d, s, m).start()

    rs_step(0, True)

    @pl.loop(1, chips - 1)
    def _(s):
        rs_step(s, False)

    def ag_copy(d, j, t, m):
        return pltpu.make_async_remote_copy(
            src_ref=gat.at[m, d, j], dst_ref=gat.at[m, d, j], send_sem=as_sem,
            recv_sem=ar_sem.at[t, d, j], device_id=dev(nxt[d]), device_id_type=MESH)

    def spread(d, j, m):
        pltpu.make_async_remote_copy(
            src_ref=gat.at[m, d, j], dst_ref=out.at[m * 2 + core, d, j], send_sem=ps_sem,
            recv_sem=pr_sem, device_id=dev(mate), device_id_type=MESH).start()
        pltpu.make_async_copy(gat.at[m, d, j], out.at[m * 2 + core, d, j], wo_sem).start()

    for d in range(2):
        ready(d, 0)
    state = epilogue.begin(ins, outs)
    for j in range(SUB):
        for d in range(2):
            rs_copy(d, j, chips - 2, chip).wait_recv()
            v = loc[chip, d, j].astype(F32) + oth[chip, d, j].astype(F32) + arr[chips - 2, d, j].astype(F32)
            res, state = epilogue.piece(v.astype(BF).astype(F32), d, j, ins, outs, state)
            gat[chip, d, j] = res
            ag_copy(d, j, 0, chip).start()
            spread(d, j, chip)
    epilogue.end(outs, state)

    if with_gain:
        for d in range(2):
            kswap(d, 0).wait_recv()
            krs_copy(d, chips - 2, chip).wait_recv()
            kout[chip * 2 + core, d] = kin[chip * 2 + core, d] + koth[chip, d] + karr[chips - 2, d]
            kag_copy(d, 0, chip).start()
            kspread(d, chip)

        def gain_copy(t, src):
            return pltpu.make_async_remote_copy(
                src_ref=src, dst_ref=gbuf.at[t], send_sem=gs_sem.at[t],
                recv_sem=gr_sem.at[t], device_id=dev(nxt[0]), device_id_type=MESH)

        gacc[0:1] = ins[4][...]
        gacc[1:2] = state
        gain_copy(0, gacc).start()

    def ag_step(t, last):
        for j in range(SUB):
            for d in range(2):
                m = chunk_at(d, t)
                ag_copy(d, j, t - 1, m).wait_recv()
                if not last:
                    ag_copy(d, j, t, m).start()
                spread(d, j, m)
        if with_gain:
            for d in range(2):
                m = chunk_at(d, t)
                kag_copy(d, t - 1, m).wait_recv()
                if not last:
                    kag_copy(d, t, m).start()
                kspread(d, m)
            gain_copy(t - 1, gacc).wait_recv()
            if not last:
                gain_copy(t, gbuf.at[t - 1]).start()

    @pl.loop(1, chips - 1)
    def _(t):
        ag_step(t, False)

    ag_step(chips - 1, True)

    if with_gain:
        tot = gacc[...]
        for t in range(chips - 1):
            tot = tot + gbuf[t]
            gain_copy(t, gacc).wait_send()
        outs[0][...] = tot
        mate_copy = pltpu.make_async_remote_copy(
            src_ref=outs[0], dst_ref=gmate, send_sem=gms_sem, recv_sem=gmr_sem,
            device_id=dev(mate), device_id_type=MESH)
        mate_copy.start()
        mate_copy.wait()
        outs[0][...] = tot + gmate[...]

    def bulk(ref, sem, rsem):
        return pltpu.make_async_remote_copy(
            src_ref=ref, dst_ref=ref, send_sem=sem, recv_sem=rsem, device_id=dev(mate), device_id_type=MESH)

    if with_gain:
        bulk(koth, kps, kpr).wait_recv()
        bulk(koth, kxs, kpr).wait_send()
        bulk(karr, krs, kpr).wait_send()
        bulk(karr, kas, kpr).wait_send()
        bulk(koth, kps, kpr).wait_send()
    bulk(gat, ps_sem, pr_sem).wait_recv()
    bulk(oth, xs_sem, pr_sem).wait_send()
    bulk(arr, rs_sem, pr_sem).wait_send()
    bulk(arr, as_sem, pr_sem).wait_send()
    bulk(gat, ps_sem, pr_sem).wait_send()
    pltpu.make_async_copy(gat, gat, wo_sem).wait()


class AddTail:
    @staticmethod
    def begin(ins, outs):
        return None

    @staticmethod
    def piece(v, d, j, ins, outs, state):
        return (ins[0][d, j].astype(F32) + v).astype(BF), state

    @staticmethod
    def end(outs, state):
        pass


class AttnTail:
    @staticmethod
    def begin(ins, outs):
        return jnp.zeros(ins[2].shape, F32)

    @staticmethod
    def piece(v, d, j, ins, outs, state):
        normed, inv = rms_parts(ins[0][d, j])
        state = state + jnp.sum(v * normed, axis=0, keepdims=True)
        grad = ins[1][d, j] + rms_back(v, normed, inv, ins[2][...])
        return grad.astype(BF), state

    @staticmethod
    def end(outs, state):
        pass


def ring_call(part, ins, out_shapes, epilogue, chips, cid, with_gain=False):
    tokens, width = part.shape
    shape = (chips * 2, 2, SUB, ROWS, width)
    half = (chips, 2, SUB, ROWS, width)
    arrive = (chips - 1, 2, SUB, ROWS, width)
    vm = pl.BlockSpec(memory_space=pltpu.VMEM)
    anyspec = pl.BlockSpec(memory_space=pl.ANY)
    dma = pltpu.SemaphoreType.DMA
    scratch = [
        pltpu.VMEM(half, BF), pltpu.VMEM(half, BF), pltpu.VMEM(arrive, BF), pltpu.VMEM(half, BF),
        dma((chips, 2)), dma, dma((chips, 2)), dma, dma((chips - 1, 2, SUB)), dma,
        dma((chips - 1, 2, SUB)), dma, dma, dma]
    if with_gain:
        scratch += [pltpu.VMEM((2, width), F32), pltpu.VMEM((chips - 1, 2, width), F32), pltpu.VMEM((2, width), F32),
                    dma((chips - 1,)), dma((chips - 1,)), dma, dma]
        kshape = ins[5].shape[1:]
        scratch += [pltpu.VMEM((chips,) + kshape, F32), pltpu.VMEM((chips,) + kshape, F32), pltpu.VMEM((chips - 1,) + kshape, F32),
                    dma, dma((chips, 2)), dma, dma((chips - 1, 2)), dma, dma((chips - 1, 2)), dma, dma]
    n_in, n_out = len(ins), len(out_shapes)

    def body(*refs):
        ring_kernel(chips, n_in, n_out, epilogue, with_gain, *refs)

    res = pl.pallas_call(
        body,
        out_shape=[jax.ShapeDtypeStruct(shape, BF)] + out_shapes,
        in_specs=[anyspec] + [vm] * n_in,
        out_specs=[anyspec] + [vm] * n_out,
        scratch_shapes=scratch,
        name='ring_%d' % cid,
        compiler_params=pltpu.CompilerParams(collective_id=cid, has_side_effects=True, vmem_limit_bytes=VMEM_LIMIT),
        cost_estimate=pl.CostEstimate(flops=80_000_000_000, bytes_accessed=4 * tokens * width, transcendentals=0),
    )(part.reshape(shape), *ins)
    return (res[0].reshape(tokens, width),) + tuple(res[1:])


def masked_probs(q, k, seg_ref, b, row0):
    n = q.shape[0]
    seg_k = seg_ref[pl.ds(b, 1), :].astype(F32)
    own = seg_ref[pl.ds(b, 1), pl.ds(row0, n)].astype(F32)
    seg_q = jnp.transpose(jnp.broadcast_to(own, (128, n)))[:, :1]
    s = mm_nt(q, k) * HEAD_DIM ** -0.5
    rows = row0 + lax.broadcasted_iota(jnp.int32, s.shape, 0)
    cols = lax.broadcasted_iota(jnp.int32, s.shape, 1)
    s = jnp.where((rows >= cols) & (seg_q == seg_k), s, -1e30)
    e = jnp.exp(s - jnp.max(s, axis=-1, keepdims=True))
    return e * (1.0 / jnp.sum(e, axis=-1, keepdims=True))


def pack(w_ref, wq_ref, wk_ref, wv_ref):
    for n, ref in enumerate((wq_ref, wk_ref, wv_ref)):
        w_ref[:, n * HEAD_DIM:(n + 1) * HEAD_DIM] = ref[...]


def front_kernel(x_ref, sg_ref, g_ref, wq_ref, wk_ref, wv_ref, wo_ref, o_ref, qkv_ref, ctx_ref, k_s, v_s, w_ref):
    qi = pl.program_id(1)

    @pl.when((qi == 0) & (pl.program_id(0) == 0))
    def _():
        k_s[...] = jnp.zeros_like(k_s)
        v_s[...] = jnp.zeros_like(v_s)
        pack(w_ref, wq_ref, wk_ref, wv_ref)

    normed, _ = rms_parts(x_ref[0])
    a = (normed * g_ref[...]).astype(BF)
    qkv = mm(a, w_ref[...]).astype(BF)
    qkv_ref[0] = qkv
    row0 = pl.multiple_of(qi * BLK, BLK)
    k_s[pl.ds(row0, BLK)] = qkv[:, HEAD_DIM:2 * HEAD_DIM]
    v_s[pl.ds(row0, BLK)] = qkv[:, 2 * HEAD_DIM:]
    probs = masked_probs(qkv[:, :HEAD_DIM], k_s[...], sg_ref, pl.program_id(0), row0)
    ctx = mm(probs.astype(BF), v_s[...]).astype(BF)
    ctx_ref[0] = ctx
    o_ref[0] = mm(ctx, wo_ref[...]).astype(BF)


def front_call(x, seg, gain, w_q, w_k, w_v, w_o):
    nb, seq, width = x.shape
    e3 = 3 * HEAD_DIM
    rowblk = lambda n: pl.BlockSpec((1, BLK, n), lambda b, i: (b, i, 0))
    whole = lambda arr: pl.BlockSpec(arr.shape, lambda b, i: (0, 0))
    return pl.pallas_call(
        front_kernel,
        grid=(nb, seq // BLK),
        in_specs=[rowblk(width), whole(seg), whole(gain), whole(w_q), whole(w_k), whole(w_v), whole(w_o)],
        out_specs=[rowblk(width), rowblk(e3), rowblk(HEAD_DIM)],
        out_shape=[jax.ShapeDtypeStruct((nb, seq, width), BF), jax.ShapeDtypeStruct((nb, seq, e3), BF),
                   jax.ShapeDtypeStruct((nb, seq, HEAD_DIM), BF)],
        scratch_shapes=[pltpu.VMEM((seq, HEAD_DIM), BF), pltpu.VMEM((seq, HEAD_DIM), BF), pltpu.VMEM((width, e3), BF)],
        name='front',
        compiler_params=pltpu.CompilerParams(vmem_limit_bytes=VMEM_LIMIT),
        cost_estimate=pl.CostEstimate(flops=8_000_000_000, bytes_accessed=20_000_000, transcendentals=0),
    )(x, seg, gain, w_q, w_k, w_v, w_o)


def back_kernel(dr_ref, x_ref, sg_ref, g_ref, wq_ref, wk_ref, wv_ref, wo_ref, q_ref, qkv_ref, ctx_ref,
                y_in, dg_in, du_in, dd_in, ga_ref, dwq_ref, dkv_ref, dwo_ref, y_ref, dg_ref, du_ref, dd_ref, dqkv_s, dk_s, dv_s, w_ref):
    b, ph = pl.program_id(0), pl.program_id(1)
    nq = pl.num_programs(1) // 2
    scale = HEAD_DIM ** -0.5
    for src, dst in ((y_in, y_ref), (dg_in, dg_ref), (du_in, du_ref), (dd_in, dd_ref)):
        dst[...] = src[...]

    @pl.when((ph == 0) & (b == 0))
    def _():
        pack(w_ref, wq_ref, wk_ref, wv_ref)
        dwq_ref[...] = jnp.zeros_like(dwq_ref)
        dkv_ref[...] = jnp.zeros_like(dkv_ref)
        dwo_ref[...] = jnp.zeros_like(dwo_ref)

    @pl.when(ph == 0)
    def _():
        dk_s[...] = jnp.zeros_like(dk_s)
        dv_s[...] = jnp.zeros_like(dv_s)

    @pl.when(ph < nq)
    def _():
        row0 = pl.multiple_of(ph * BLK, BLK)
        dr = dr_ref[0]
        dctx = mm_nt(dr, wo_ref[...]).astype(BF)
        dwo_ref[...] += mm_tn(ctx_ref[0], dr)
        q = q_ref[0]
        k = qkv_ref[0, :, HEAD_DIM:2 * HEAD_DIM]
        v = qkv_ref[0, :, 2 * HEAD_DIM:]
        probs = masked_probs(q, k, sg_ref, b, row0)
        dp = mm_nt(dctx, v)
        ds = (probs * (dp - jnp.sum(dp * probs, axis=-1, keepdims=True)) * scale).astype(BF)
        dv_s[...] += mm_tn(probs.astype(BF), dctx)
        dk_s[...] += mm_tn(ds, q)
        dqkv_s[pl.ds(row0, BLK), :HEAD_DIM] = mm(ds, k).astype(BF)

    @pl.when(ph == nq - 1)
    def _():
        dqkv_s[:, HEAD_DIM:2 * HEAD_DIM] = dk_s[...].astype(BF)
        dqkv_s[:, 2 * HEAD_DIM:] = dv_s[...].astype(BF)

    @pl.when(ph >= nq)
    def _():
        row0 = pl.multiple_of((ph - nq) * BLK, BLK)
        normed, _ = rms_parts(x_ref[0])
        a = (normed * g_ref[...]).astype(BF)
        blk = dqkv_s[pl.ds(row0, BLK)]
        dw = mm_tn(a, blk)
        dwq_ref[...] += dw[:, :HEAD_DIM]
        dkv_ref[...] += dw[:, HEAD_DIM:]
        ga_ref[0] = mm_nt(blk, w_ref[...]).astype(BF)


def back_call(dr, x, seg, gain, w_q, w_k, w_v, w_o, qkv, ctx, carried):
    nb, seq, width = x.shape
    nq = seq // BLK
    e3 = 3 * HEAD_DIM
    first = lambda n: pl.BlockSpec((1, BLK, n), lambda b, i: (b, jnp.minimum(i, nq - 1), 0))
    second = lambda n: pl.BlockSpec((1, BLK, n), lambda b, i: (b, jnp.maximum(i - nq, 0), 0))
    whole = lambda arr: pl.BlockSpec(arr.shape, lambda b, i: (0, 0))
    const = lambda shp: pl.BlockSpec(shp, lambda b, i: (0, 0))
    n_steps = nb * 2 * nq
    y, grads = carried[0], carried[1:]
    thru = [pl.BlockSpec((y.shape[0] // n_steps, width), lambda b, i: (b * 2 * nq + i, 0))]
    thru += [pl.BlockSpec((g.shape[0], width // n_steps), lambda b, i: (0, b * 2 * nq + i)) for g in grads]
    return pl.pallas_call(
        back_kernel,
        grid=(nb, 2 * nq),
        in_specs=[first(width), second(width), whole(seg), whole(gain), whole(w_q), whole(w_k), whole(w_v), whole(w_o),
                  first(HEAD_DIM), pl.BlockSpec((1, seq, e3), lambda b, i: (b, 0, 0)), first(HEAD_DIM)] + thru,
        out_specs=[second(width), const((width, HEAD_DIM)), const((width, 2 * HEAD_DIM)), const((HEAD_DIM, width))] + thru,
        out_shape=[jax.ShapeDtypeStruct((nb, seq, width), BF), jax.ShapeDtypeStruct((width, HEAD_DIM), F32),
                   jax.ShapeDtypeStruct((width, 2 * HEAD_DIM), F32),
                   jax.ShapeDtypeStruct((HEAD_DIM, width), F32)] + [jax.ShapeDtypeStruct(c.shape, c.dtype) for c in carried],
        scratch_shapes=[pltpu.VMEM((seq, e3), BF), pltpu.VMEM((seq, HEAD_DIM), F32), pltpu.VMEM((seq, HEAD_DIM), F32), pltpu.VMEM((width, e3), BF)],
        name='back',
        compiler_params=pltpu.CompilerParams(vmem_limit_bytes=VMEM_LIMIT),
        cost_estimate=pl.CostEstimate(flops=12_000_000_000, bytes_accessed=30_000_000, transcendentals=0),
    )(dr, x, seg, gain, w_q, w_k, w_v, w_o, qkv, qkv, ctx, *carried)


def mid_kernel(chips, part, x, dy, g_ref, wg, wu, wd, out, p_out, h_own, x_own, dres_own, gpart, dwg, dwu, dwd,
               loc, oth, arr, gat, gat2, dyb, pst, gst, dy_own,
               ld_sem, xs_sem, xr_sem, rs_sem, rr_sem, as_sem, ar_sem, ps_sem, pm_sem, own_sem, dy_sem, po_sem,
               xs2_sem, xr2_sem, rs2_sem, rr2_sem, as2_sem, ar2_sem, ps2_sem, pr2_sem, wo_sem):
    me = lax.axis_index('tp')
    chip = me // 2
    core = me % 2
    mate = chip * 2 + 1 - core
    nxt = (lax.rem(chip + 1, chips) * 2 + core, lax.rem(chip + chips - 1, chips) * 2 + core)
    width = x.shape[-1]
    last = chips - 1

    def remote(src, dst, ssem, rsem, t):
        return pltpu.make_async_remote_copy(src_ref=src, dst_ref=dst, send_sem=ssem, recv_sem=rsem,
                                            device_id={'tp': t}, device_id_type=MESH)

    barrier = pltpu.get_barrier_semaphore()
    for t in (nxt[0], nxt[1], mate):
        pl.semaphore_signal(barrier, inc=1, device_id={'tp': t}, device_id_type=MESH)
    pl.semaphore_wait(barrier, 3)

    def chunk_at(d, s):
        return lax.rem(chip + (s if d == 1 else chips - s), chips)

    def swap(d, s):
        m = chunk_at(d, s)
        return remote(part.at[m * 2 + 1 - core, d], oth.at[m, d], xs_sem, xr_sem.at[m, d], mate)

    def load(d, s):
        m = chunk_at(d, s)
        return pltpu.make_async_copy(part.at[m * 2 + core, d], loc.at[m, d], ld_sem.at[m, d])

    def dy_copy(d, t):
        m = chunk_at(d, t)
        return pltpu.make_async_copy(dy.at[pl.ds(m * 2, 2), d], dyb.at[t % 2, d], dy_sem.at[t % 2, d])

    for s in range(1, chips + 1):
        for d in range(2):
            swap(d, s % chips).start()
            load(d, s % chips).start()
    x_load = pltpu.make_async_copy(x.at[me], x_own, own_sem.at[0])
    dy_load = pltpu.make_async_copy(dy.at[me], dy_own, own_sem.at[1])
    x_load.start()
    dy_load.start()
    for d in range(2):
        dy_copy(d, 0).start()
    for acc in (dwg, dwu, dwd):
        acc[...] = jnp.zeros_like(acc)

    def rs_copy(d, j, s, m, ssem, rsem):
        return remote(loc.at[m, d, j], arr.at[s, d, j], ssem, rsem.at[s, d, j], nxt[d])

    def rs_step(s, first):
        for d in range(2):
            load(d, s + 1).wait()
            swap(d, s + 1).wait_recv()
        for j in range(SUB):
            for d in range(2):
                m = chunk_at(d, s + 1)
                v = loc[m, d, j].astype(F32) + oth[m, d, j].astype(F32)
                if not first:
                    rs_copy(d, j, s - 1, m, rs_sem, rr_sem).wait_recv()
                    v = v + arr[s - 1, d, j].astype(F32)
                loc[m, d, j] = v.astype(BF)
                rs_copy(d, j, s, m, rs_sem, rr_sem).start()

    rs_step(0, True)

    @pl.loop(1, last)
    def _(s):
        rs_step(s, False)

    def ag_copy(d, j, t, m):
        return remote(gat.at[m * 2 + core, d, j], gat.at[m * 2 + core, d, j], as_sem, ar_sem.at[t, d, j], nxt[d])

    def spread(d, j, t, m):
        remote(gat.at[m * 2 + core, d, j], gat.at[m * 2 + core, d, j], ps_sem, pm_sem.at[t], mate).start()

    x_load.wait()
    dy_load.wait()
    for d in range(2):
        load(d, 0).wait()
        swap(d, 0).wait_recv()
    for j in range(SUB):
        for d in range(2):
            rs_copy(d, j, last - 1, chip, rs_sem, rr_sem).wait_recv()
            v = loc[chip, d, j].astype(F32) + oth[chip, d, j].astype(F32) + arr[last - 1, d, j].astype(F32)
            h = (x_own[d, j].astype(F32) + v.astype(BF).astype(F32)).astype(BF)
            h_own[d, j] = h
            normed, _ = rms_parts(h)
            gat[me, d, j] = (normed * g_ref[...]).astype(BF)
            ag_copy(d, j, 0, chip).start()
            spread(d, j, 0, chip)

    def bulk(ref, sem, rsem):
        return remote(ref, ref, sem, rsem, mate)

    bulk(arr, rs_sem, pr2_sem).wait_send()

    def p_copy(d, t):
        m = chunk_at(d, t)
        return pltpu.make_async_copy(pst.at[t % 2, d], p_out.at[pl.ds(m * 2, 2), d], po_sem.at[t % 2, d])

    def swap2(d, t):
        m = chunk_at(d, t)
        return remote(gst.at[t % 2, d, 1 - core], oth.at[m, d], xs2_sem.at[t % 2, d], xr2_sem.at[m, d], mate)

    def rs2_step(t, first):
        slot = t % 2
        for d in range(2):
            swap2(d, t).wait_recv()
        for j in range(SUB):
            for d in range(2):
                m = chunk_at(d, t)
                v = gst[slot, d, core, j].astype(F32) + oth[m, d, j].astype(F32)
                if not first:
                    rs_copy(d, j, t - 2, m, rs2_sem, rr2_sem).wait_recv()
                    v = v + arr[t - 2, d, j].astype(F32)
                loc[m, d, j] = v.astype(BF)
                rs_copy(d, j, t - 1, m, rs2_sem, rr2_sem).start()

    def collect(t, onward):
        for j in range(SUB):
            for d in range(2):
                m = chunk_at(d, t)
                ag_copy(d, j, t - 1, m).wait_recv()
                if onward:
                    ag_copy(d, j, t, m).start()
                spread(d, j, t, m)

    step = width // 4

    @pl.loop(0, chips)
    def _(t):
        slot = t % 2
        a = chunk_at(0, t)
        b = chunk_at(1, t)

        @pl.when((t > 0) & (t < last))
        def _():
            collect(t, True)

        @pl.when(t == last)
        def _():
            collect(t, False)

        @pl.when(t < last)
        def _():
            for d in range(2):
                dy_copy(d, t + 1).start()

        @pl.when(t >= 2)
        def _():
            for d in range(2):
                p_copy(d, t - 2).wait()
                swap2(d, t - 2).wait_send()

        for d in range(2):
            dy_copy(d, t).wait()
        bulk(gat.at[0], ps_sem, pm_sem.at[t]).wait_recv()

        rows = 4 * SUB * ROWS
        mb = jnp.concatenate([gat[pl.ds(a * 2, 2), 0].reshape(rows // 2, width), gat[pl.ds(b * 2, 2), 1].reshape(rows // 2, width)], axis=0)
        dyv = dyb[slot].reshape(rows, width)
        gate = mm_nt(mb, wg[...])
        upper = mm_nt(mb, wu[...])
        dact = mm_nt(dyv, wd[...])
        sig = jax.nn.sigmoid(gate)
        act = (gate * sig * upper).astype(BF)
        dgate = (dact * upper * sig * (1.0 + gate * (1.0 - sig))).astype(BF)
        dupper = (dact * gate * sig).astype(BF)
        for n in range(4):
            cs = slice(n * step, (n + 1) * step)
            gst[slot, :, :, :, :, cs] = (mm(dgate, wg[:, cs]) + mm(dupper, wu[:, cs])).astype(BF).reshape(2, 2, SUB, ROWS, step)
        for d in range(2):
            swap2(d, t).start()
        for n in range(4):
            cs = slice(n * step, (n + 1) * step)
            pst[slot, :, :, :, :, cs] = mm(act, wd[:, cs]).astype(BF).reshape(2, 2, SUB, ROWS, step)
            dwd[:, cs] += mm_tn(act, dyv[:, cs])
            dwg[:, cs] += mm_tn(dgate, mb[:, cs])
            dwu[:, cs] += mm_tn(dupper, mb[:, cs])
        for d in range(2):
            p_copy(d, t).start()

        @pl.when(t == 0)
        def _():
            for d in range(2):
                loc[chip, d] = gst[0, d, core]

        @pl.when(t == 1)
        def _():
            rs2_step(t, True)

        @pl.when(t > 1)
        def _():
            rs2_step(t, False)

    def ag2_copy(d, j, t, m):
        return remote(gat2.at[m, d, j], gat2.at[m, d, j], as2_sem, ar2_sem.at[t, d, j], nxt[d])

    def spread2(d, j, m):
        remote(gat2.at[m, d, j], out.at[m * 2 + core, d, j], ps2_sem, pr2_sem, mate).start()
        pltpu.make_async_copy(gat2.at[m, d, j], out.at[m * 2 + core, d, j], wo_sem).start()

    for d in range(2):
        swap2(d, 0).wait_recv()
    total = jnp.zeros((1, width), F32)
    for j in range(SUB):
        for d in range(2):
            rs_copy(d, j, last - 1, chip, rs2_sem, rr2_sem).wait_recv()
            v = loc[chip, d, j].astype(F32) + oth[chip, d, j].astype(F32) + arr[last - 1, d, j].astype(F32)
            v = v.astype(BF).astype(F32)
            normed, inv = rms_parts(h_own[d, j])
            total = total + jnp.sum(v * normed, axis=0, keepdims=True)
            grad = dy_own[d, j].astype(F32) + rms_back(v, normed, inv, g_ref[...])
            dres_own[d, j] = grad
            gat2[chip, d, j] = grad.astype(BF)
            ag2_copy(d, j, 0, chip).start()
            spread2(d, j, chip)
    gpart[...] = total

    def ag2_step(t, onward):
        for j in range(SUB):
            for d in range(2):
                m = chunk_at(d, t)
                ag2_copy(d, j, t - 1, m).wait_recv()
                if onward:
                    ag2_copy(d, j, t, m).start()
                spread2(d, j, m)

    @pl.loop(1, last)
    def _(t):
        ag2_step(t, True)

    ag2_step(last, False)

    bulk(gat2, ps2_sem, pr2_sem).wait_recv()
    for sem in (xs_sem, ps_sem, ps2_sem):
        bulk(oth, sem, pr2_sem).wait_send()
    for sem in (as_sem, rs2_sem, as2_sem):
        bulk(arr, sem, pr2_sem).wait_send()
    for t in (chips - 2, chips - 1):
        for d in range(2):
            p_copy(d, t).wait()
            swap2(d, t).wait_send()
    pltpu.make_async_copy(gat2, gat2, wo_sem).wait()


def mid_call(part, x, dy, gain, w_gate, w_up, w_down, chips, cid):
    tokens, width = part.shape
    ff = w_down.shape[0]
    shape = (chips * 2, 2, SUB, ROWS, width)
    half = (chips, 2, SUB, ROWS, width)
    arrive = (chips - 1, 2, SUB, ROWS, width)
    piece = (2, SUB, ROWS, width)
    pair = (2, 2, 2, SUB, ROWS, width)
    vm = pl.BlockSpec(memory_space=pltpu.VMEM)
    anyspec = pl.BlockSpec(memory_space=pl.ANY)
    dma = pltpu.SemaphoreType.DMA
    steps = dma((chips - 1, 2, SUB))
    vmb = lambda shp: pltpu.VMEM(shp, BF)
    grad = jax.ShapeDtypeStruct((ff, width), F32)
    res = pl.pallas_call(
        functools.partial(mid_kernel, chips),
        out_shape=[jax.ShapeDtypeStruct(shape, BF), jax.ShapeDtypeStruct(shape, BF), jax.ShapeDtypeStruct(piece, BF),
                   jax.ShapeDtypeStruct(piece, BF), jax.ShapeDtypeStruct(piece, F32), jax.ShapeDtypeStruct((1, width), F32),
                   grad, grad, grad],
        in_specs=[anyspec] * 3 + [vm] * 4,
        out_specs=[anyspec] * 2 + [vm] * 7,
        scratch_shapes=[
            vmb(half), vmb(half), vmb(arrive), vmb(shape), vmb(half), vmb(pair), vmb(pair), vmb(pair), vmb(piece),
            dma((chips, 2)), dma, dma((chips, 2)), dma, steps, dma, steps, dma, dma((chips,)), dma((2,)), dma((2, 2)), dma((2, 2)),
            dma((2, 2)), dma((chips, 2)), dma, steps, dma, steps, dma, dma, dma],
        name='middle',
        compiler_params=pltpu.CompilerParams(collective_id=cid, has_side_effects=True, vmem_limit_bytes=67_000_000),
        cost_estimate=pl.CostEstimate(flops=120_000_000_000, bytes_accessed=40 * tokens * width, transcendentals=0),
    )(part.reshape(shape), x.reshape(shape), dy.reshape(shape), gain, w_gate, w_up, w_down)
    return (res[0].reshape(tokens, width), res[1].reshape(tokens, width)) + tuple(res[2:])


def solution(mesh):
    tp_size = mesh.shape['tp']
    chips = tp_size // 2

    def device_step(hidden, seg_ids, grad_out, gain_attn, gain_mlp, w_q, w_k, w_v, w_o, w_gate, w_up, w_down):
        nb, seq, width = hidden.shape
        tokens = nb * seq
        own = tokens // tp_size
        g1 = gain_attn[None, :]
        g2 = gain_mlp[None, :]
        weights = (w_q, w_k, w_v, w_o)

        o_part, qkv, ctx = front_call(hidden, seg_ids, g1, *weights)
        dres, p_part, h_own, x_own, dres_own, g2_part, d_gate, d_up, d_down = mid_call(
            o_part.reshape(tokens, width), hidden, grad_out, g2, w_gate.T, w_up.T, w_down, chips, 1)
        (y_out,) = ring_call(p_part, [h_own], [], AddTail, chips, 4)
        ga_part, d_q, d_kv, d_o, y_out, d_gate, d_up, d_down = back_call(
            dres.reshape(nb, seq, width), hidden, seg_ids, g1, *weights, qkv, ctx, (y_out, d_gate, d_up, d_down))
        kv_rows = own // 2
        kv_shape = (tp_size, 2, kv_rows, 2 * HEAD_DIM)
        dx, gains, d_kv = ring_call(ga_part.reshape(tokens, width), [x_own, dres_own, g1, g1, g2_part, d_kv.reshape(kv_shape)],
                                    [jax.ShapeDtypeStruct((2, width), F32), jax.ShapeDtypeStruct(kv_shape, F32)], AttnTail, chips, 3, True)
        d_kv = d_kv.reshape(width, 2 * HEAD_DIM)
        return (y_out.reshape(nb, seq, width), dx.reshape(nb, seq, width), gains[1], gains[0], d_q, d_kv[:, :HEAD_DIM], d_kv[:, HEAD_DIM:],
                d_o, d_gate.T, d_up.T, d_down)

    spec_act = P('data', None, None)
    spec_rows = P('data', None)
    spec_gain = P(None)
    spec_cols = P(None, 'tp')
    spec_tprows = P('tp', None)
    spec_whole = P(None, None)
    spec_stack = P(('data', 'tp'), None)
    in_specs = (spec_act, spec_rows, spec_act, spec_gain, spec_gain, spec_cols, spec_whole, spec_whole, spec_tprows, spec_cols, spec_cols, spec_tprows)
    out_specs = (spec_act, spec_act, P('data'), P('data'), P('data', 'tp'), spec_rows, spec_rows, spec_stack, P('data', 'tp'), P('data', 'tp'), spec_stack)
    return jax.shard_map(device_step, mesh=mesh, in_specs=in_specs, out_specs=out_specs, check_vma=False)
```

```python
import functools
import jax
import jax.numpy as jnp
from jax import lax
from jax.experimental import pallas as pl
from jax.experimental.pallas import tpu as pltpu
from jax.sharding import PartitionSpec as P

HEAD_DIM = 128
EPS = 1e-5
SUB = 4
ROWS = 16
BLK = 256
BF = jnp.bfloat16
F32 = jnp.float32
MESH = pl.DeviceIdType.MESH
VMEM_LIMIT = 60 * 1024 * 1024


def mm(a, b):
    return lax.dot_general(a, b, (((1,), (0,)), ((), ())), preferred_element_type=F32)


def mm_nt(a, b):
    return lax.dot_general(a, b, (((1,), (1,)), ((), ())), preferred_element_type=F32)


def mm_tn(a, b):
    return lax.dot_general(a, b, (((0,), (0,)), ((), ())), preferred_element_type=F32)


def rms_parts(x_in):
    x_float = x_in.astype(F32)
    inv = lax.rsqrt(jnp.mean(x_float * x_float, axis=-1, keepdims=True) + EPS)
    return x_float * inv, inv


def rms_back(grad, normed, inv, gain):
    scaled = grad * gain
    return inv * (scaled - normed * jnp.mean(scaled * normed, axis=-1, keepdims=True))


def ring_kernel(chips, n_in, n_out, epilogue, with_gain, task, part, *refs):
    ins = refs[:n_in]
    out = refs[n_in]
    outs = refs[n_in + 1:n_in + 1 + n_out]
    scratch = refs[n_in + 1 + n_out:]
    (loc, oth, arr, gat, ld_sem, xs_sem, xr_sem, rs_sem, rr_sem, as_sem, ar_sem, ps_sem, pr_sem, wo_sem) = scratch[:14]
    me = lax.axis_index('tp')
    chip = me // 2
    core = me % 2
    mate = chip * 2 + 1 - core
    nxt = (lax.rem(chip + 1, chips) * 2 + core, lax.rem(chip + chips - 1, chips) * 2 + core)

    def dev(t):
        return {'tp': t}

    barrier = pltpu.get_barrier_semaphore()
    for t in (nxt[0], nxt[1], mate):
        pl.semaphore_signal(barrier, inc=1, device_id=dev(t), device_id_type=MESH)
    pl.semaphore_wait(barrier, 3)

    def chunk_at(d, s):
        off = s if d == 1 else chips - s
        return lax.rem(chip + off, chips)

    def swap(d, s):
        m = chunk_at(d, s)
        return pltpu.make_async_remote_copy(
            src_ref=part.at[m * 2 + 1 - core, d], dst_ref=oth.at[m, d], send_sem=xs_sem,
            recv_sem=xr_sem.at[m, d], device_id=dev(mate), device_id_type=MESH)

    def load(d, s):
        m = chunk_at(d, s)
        return pltpu.make_async_copy(part.at[m * 2 + core, d], loc.at[m, d], ld_sem.at[m, d])

    if with_gain:
        (gacc, gbuf, gmate, gs_sem, gr_sem, gms_sem, gmr_sem, kacc, koth, karr, kxs, kxr, krs, krr, kas, kar, kps, kpr) = scratch[14:]
        kin, kout = ins[5], outs[1]

        def kswap(d, s):
            m = chunk_at(d, s)
            return pltpu.make_async_remote_copy(
                src_ref=kin.at[m * 2 + 1 - core, d], dst_ref=koth.at[m, d], send_sem=kxs,
                recv_sem=kxr.at[m, d], device_id=dev(mate), device_id_type=MESH)

        def krs_copy(d, s, m):
            return pltpu.make_async_remote_copy(
                src_ref=kacc.at[m, d], dst_ref=karr.at[s, d], send_sem=krs,
                recv_sem=krr.at[s, d], device_id=dev(nxt[d]), device_id_type=MESH)

        def kag_copy(d, t, m):
            return pltpu.make_async_remote_copy(
                src_ref=kout.at[m * 2 + core, d], dst_ref=kout.at[m * 2 + core, d], send_sem=kas,
                recv_sem=kar.at[t, d], device_id=dev(nxt[d]), device_id_type=MESH)

        def kspread(d, m):
            pltpu.make_async_remote_copy(
                src_ref=kout.at[m * 2 + core, d], dst_ref=kout.at[m * 2 + core, d], send_sem=kps,
                recv_sem=kpr, device_id=dev(mate), device_id_type=MESH).start()

    for s in range(1, chips + 1):
        for d in range(2):
            swap(d, s % chips).start()
            load(d, s % chips).start()
            if with_gain:
                kswap(d, s % chips).start()

    def rs_copy(d, j, s, m):
        return pltpu.make_async_remote_copy(
            src_ref=loc.at[m, d, j], dst_ref=arr.at[s, d, j], send_sem=rs_sem,
            recv_sem=rr_sem.at[s, d, j], device_id=dev(nxt[d]), device_id_type=MESH)

    def ready(d, s):
        load(d, s).wait()
        swap(d, s).wait_recv()

    def rs_step(s, first):
        for d in range(2):
            ready(d, s + 1)
        for j in range(SUB):
            for d in range(2):
                m = chunk_at(d, s + 1)
                v = loc[m, d, j].astype(F32) + oth[m, d, j].astype(F32)
                if not first:
                    rs_copy(d, j, s - 1, m).wait_recv()
                    v = v + arr[s - 1, d, j].astype(F32)
                loc[m, d, j] = v.astype(BF)
                rs_copy(d, j, s, m).start()
        if with_gain:
            for d in range(2):
                m = chunk_at(d, s + 1)
                kswap(d, s + 1).wait_recv()
                kv = kin[m * 2 + core, d] + koth[m, d]
                if not first:
                    krs_copy(d, s - 1, m).wait_recv()
                    kv = kv + karr[s - 1, d]
                kacc[m, d] = kv
                krs_copy(d, s, m).start()

    rs_step(0, True)

    if task:
        work, work_end, work_count = task(ins, outs, scratch[14:])

    def work_share(n):
        if task:
            span = 2 * (chips - 2)
            pl.loop(n * work_count // span, (n + 1) * work_count // span)(work)

    @pl.loop(1, chips - 1)
    def _(s):
        rs_step(s, False)
        work_share(s - 1)

    def ag_copy(d, j, t, m):
        return pltpu.make_async_remote_copy(
            src_ref=gat.at[m, d, j], dst_ref=gat.at[m, d, j], send_sem=as_sem,
            recv_sem=ar_sem.at[t, d, j], device_id=dev(nxt[d]), device_id_type=MESH)

    def spread(d, j, m):
        pltpu.make_async_remote_copy(
            src_ref=gat.at[m, d, j], dst_ref=out.at[m * 2 + core, d, j], send_sem=ps_sem,
            recv_sem=pr_sem, device_id=dev(mate), device_id_type=MESH).start()
        pltpu.make_async_copy(gat.at[m, d, j], out.at[m * 2 + core, d, j], wo_sem).start()

    for d in range(2):
        ready(d, 0)
    state = epilogue.begin(ins, outs)
    for j in range(SUB):
        for d in range(2):
            rs_copy(d, j, chips - 2, chip).wait_recv()
            v = loc[chip, d, j].astype(F32) + oth[chip, d, j].astype(F32) + arr[chips - 2, d, j].astype(F32)
            res, state = epilogue.piece(v.astype(BF).astype(F32), d, j, ins, outs, state)
            gat[chip, d, j] = res
            ag_copy(d, j, 0, chip).start()
            spread(d, j, chip)
    epilogue.end(outs, state)

    if with_gain:
        for d in range(2):
            kswap(d, 0).wait_recv()
            krs_copy(d, chips - 2, chip).wait_recv()
            kout[chip * 2 + core, d] = kin[chip * 2 + core, d] + koth[chip, d] + karr[chips - 2, d]
            kag_copy(d, 0, chip).start()
            kspread(d, chip)

        def gain_copy(t, src):
            return pltpu.make_async_remote_copy(
                src_ref=src, dst_ref=gbuf.at[t], send_sem=gs_sem.at[t],
                recv_sem=gr_sem.at[t], device_id=dev(nxt[0]), device_id_type=MESH)

        gacc[0:1] = ins[4][...]
        gacc[1:2] = state
        gain_copy(0, gacc).start()

    def ag_step(t, last):
        for j in range(SUB):
            for d in range(2):
                m = chunk_at(d, t)
                ag_copy(d, j, t - 1, m).wait_recv()
                if not last:
                    ag_copy(d, j, t, m).start()
                spread(d, j, m)
        if with_gain:
            for d in range(2):
                m = chunk_at(d, t)
                kag_copy(d, t - 1, m).wait_recv()
                if not last:
                    kag_copy(d, t, m).start()
                kspread(d, m)
            gain_copy(t - 1, gacc).wait_recv()
            if not last:
                gain_copy(t, gbuf.at[t - 1]).start()

    @pl.loop(1, chips - 1)
    def _(t):
        ag_step(t, False)
        work_share(chips - 3 + t)

    ag_step(chips - 1, True)
    if task:
        work_end()

    if with_gain:
        tot = gacc[...]
        for t in range(chips - 1):
            tot = tot + gbuf[t]
            gain_copy(t, gacc).wait_send()
        outs[0][...] = tot
        mate_copy = pltpu.make_async_remote_copy(
            src_ref=outs[0], dst_ref=gmate, send_sem=gms_sem, recv_sem=gmr_sem,
            device_id=dev(mate), device_id_type=MESH)
        mate_copy.start()
        mate_copy.wait()
        outs[0][...] = tot + gmate[...]

    def bulk(ref, sem, rsem):
        return pltpu.make_async_remote_copy(
            src_ref=ref, dst_ref=ref, send_sem=sem, recv_sem=rsem, device_id=dev(mate), device_id_type=MESH)

    if with_gain:
        bulk(koth, kps, kpr).wait_recv()
        bulk(koth, kxs, kpr).wait_send()
        bulk(karr, krs, kpr).wait_send()
        bulk(karr, kas, kpr).wait_send()
        bulk(koth, kps, kpr).wait_send()
    bulk(gat, ps_sem, pr_sem).wait_recv()
    bulk(oth, xs_sem, pr_sem).wait_send()
    bulk(arr, rs_sem, pr_sem).wait_send()
    bulk(arr, as_sem, pr_sem).wait_send()
    bulk(gat, ps_sem, pr_sem).wait_send()
    pltpu.make_async_copy(gat, gat, wo_sem).wait()


class AddTail:
    @staticmethod
    def begin(ins, outs):
        return None

    @staticmethod
    def piece(v, d, j, ins, outs, state):
        return (ins[0][d, j].astype(F32) + v).astype(BF), state

    @staticmethod
    def end(outs, state):
        pass


class AttnTail:
    @staticmethod
    def begin(ins, outs):
        return jnp.zeros(ins[2].shape, F32)

    @staticmethod
    def piece(v, d, j, ins, outs, state):
        normed, inv = rms_parts(ins[0][d, j])
        state = state + jnp.sum(v * normed, axis=0, keepdims=True)
        grad = ins[1][d, j] + rms_back(v, normed, inv, ins[2][...])
        return grad.astype(BF), state

    @staticmethod
    def end(outs, state):
        pass


def ring_call(part, ins, out_shapes, epilogue, chips, cid, with_gain=False, task=None, in_any=(), out_any=(), extra=()):
    tokens, width = part.shape
    shape = (chips * 2, 2, SUB, ROWS, width)
    half = (chips, 2, SUB, ROWS, width)
    arrive = (chips - 1, 2, SUB, ROWS, width)
    vm = pl.BlockSpec(memory_space=pltpu.VMEM)
    anyspec = pl.BlockSpec(memory_space=pl.ANY)
    dma = pltpu.SemaphoreType.DMA
    scratch = [
        pltpu.VMEM(half, BF), pltpu.VMEM(half, BF), pltpu.VMEM(arrive, BF), pltpu.VMEM(half, BF),
        dma((chips, 2)), dma, dma((chips, 2)), dma, dma((chips - 1, 2, SUB)), dma,
        dma((chips - 1, 2, SUB)), dma, dma, dma]
    if with_gain:
        scratch += [pltpu.VMEM((2, width), F32), pltpu.VMEM((chips - 1, 2, width), F32), pltpu.VMEM((2, width), F32),
                    dma((chips - 1,)), dma((chips - 1,)), dma, dma]
        kshape = ins[5].shape[1:]
        scratch += [pltpu.VMEM((chips,) + kshape, F32), pltpu.VMEM((chips,) + kshape, F32), pltpu.VMEM((chips - 1,) + kshape, F32),
                    dma, dma((chips, 2)), dma, dma((chips - 1, 2)), dma, dma((chips - 1, 2)), dma, dma]
    scratch += list(extra)
    n_in, n_out = len(ins), len(out_shapes)

    def body(*refs):
        ring_kernel(chips, n_in, n_out, epilogue, with_gain, task, *refs)

    res = pl.pallas_call(
        body,
        out_shape=[jax.ShapeDtypeStruct(shape, BF)] + out_shapes,
        in_specs=[anyspec] + [anyspec if n in in_any else vm for n in range(n_in)],
        out_specs=[anyspec] + [anyspec if n in out_any else vm for n in range(n_out)],
        scratch_shapes=scratch,
        name='ring_%d' % cid,
        compiler_params=pltpu.CompilerParams(collective_id=cid, has_side_effects=True, vmem_limit_bytes=VMEM_LIMIT),
        cost_estimate=pl.CostEstimate(flops=80_000_000_000, bytes_accessed=4 * tokens * width, transcendentals=0),
    )(part.reshape(shape), *ins)
    return (res[0].reshape(tokens, width),) + tuple(res[1:])


def masked_probs(q, k, seg_ref, b, row0):
    n = q.shape[0]
    seg_k = seg_ref[pl.ds(b, 1), :].astype(F32)
    own = seg_ref[pl.ds(b, 1), pl.ds(row0, n)].astype(F32)
    seg_q = jnp.transpose(jnp.broadcast_to(own, (128, n)))[:, :1]
    s = mm_nt(q, k) * HEAD_DIM ** -0.5
    rows = row0 + lax.broadcasted_iota(jnp.int32, s.shape, 0)
    cols = lax.broadcasted_iota(jnp.int32, s.shape, 1)
    s = jnp.where((rows >= cols) & (seg_q == seg_k), s, -1e30)
    e = jnp.exp(s - jnp.max(s, axis=-1, keepdims=True))
    return e * (1.0 / jnp.sum(e, axis=-1, keepdims=True))


def pack(w_ref, wq_ref, wk_ref, wv_ref):
    for n, ref in enumerate((wq_ref, wk_ref, wv_ref)):
        w_ref[:, n * HEAD_DIM:(n + 1) * HEAD_DIM] = ref[...]


def front_kernel(x_ref, sg_ref, g_ref, wq_ref, wk_ref, wv_ref, wo_ref, o_ref, qkv_ref, ctx_ref, k_s, v_s, w_ref):
    qi = pl.program_id(1)

    @pl.when((qi == 0) & (pl.program_id(0) == 0))
    def _():
        k_s[...] = jnp.zeros_like(k_s)
        v_s[...] = jnp.zeros_like(v_s)
        pack(w_ref, wq_ref, wk_ref, wv_ref)

    normed, _ = rms_parts(x_ref[0])
    a = (normed * g_ref[...]).astype(BF)
    qkv = mm(a, w_ref[...]).astype(BF)
    qkv_ref[0] = qkv
    row0 = pl.multiple_of(qi * BLK, BLK)
    k_s[pl.ds(row0, BLK)] = qkv[:, HEAD_DIM:2 * HEAD_DIM]
    v_s[pl.ds(row0, BLK)] = qkv[:, 2 * HEAD_DIM:]
    probs = masked_probs(qkv[:, :HEAD_DIM], k_s[...], sg_ref, pl.program_id(0), row0)
    ctx = mm(probs.astype(BF), v_s[...]).astype(BF)
    ctx_ref[0] = ctx
    o_ref[0] = mm(ctx, wo_ref[...]).astype(BF)


def front_call(x, seg, gain, w_q, w_k, w_v, w_o):
    nb, seq, width = x.shape
    e3 = 3 * HEAD_DIM
    rowblk = lambda n: pl.BlockSpec((1, BLK, n), lambda b, i: (b, i, 0))
    whole = lambda arr: pl.BlockSpec(arr.shape, lambda b, i: (0, 0))
    return pl.pallas_call(
        front_kernel,
        grid=(nb, seq // BLK),
        in_specs=[rowblk(width), whole(seg), whole(gain), whole(w_q), whole(w_k), whole(w_v), whole(w_o)],
        out_specs=[rowblk(width), rowblk(e3), rowblk(HEAD_DIM)],
        out_shape=[jax.ShapeDtypeStruct((nb, seq, width), BF), jax.ShapeDtypeStruct((nb, seq, e3), BF),
                   jax.ShapeDtypeStruct((nb, seq, HEAD_DIM), BF)],
        scratch_shapes=[pltpu.VMEM((seq, HEAD_DIM), BF), pltpu.VMEM((seq, HEAD_DIM), BF), pltpu.VMEM((width, e3), BF)],
        name='front',
        compiler_params=pltpu.CompilerParams(vmem_limit_bytes=VMEM_LIMIT),
        cost_estimate=pl.CostEstimate(flops=8_000_000_000, bytes_accessed=20_000_000, transcendentals=0),
    )(x, seg, gain, w_q, w_k, w_v, w_o)


def back_task(ins, outs, scratch):
    dr_ref, x_ref, sg_ref, g_ref, wq_ref, wk_ref, wv_ref, wo_ref, qkv_ref, ctx_ref = ins[1:]
    ga_ref, dwq_ref, dkv_ref, dwo_ref = outs
    inb, gab, dqkv_s, dk_s, dv_s, w_ref, in_sem, ga_sem = scratch
    nb, seq, width = dr_ref.shape
    nq = seq // BLK
    count = nb * 2 * nq
    scale = HEAD_DIM ** -0.5

    def fetch(n):
        b, ph = n // (2 * nq), n % (2 * nq)
        row0 = pl.multiple_of((ph % nq) * BLK, BLK)

        @pl.when(ph < nq)
        def _():
            pltpu.make_async_copy(dr_ref.at[b, pl.ds(row0, BLK)], inb.at[n % 2], in_sem.at[n % 2]).start()

        @pl.when(ph >= nq)
        def _():
            pltpu.make_async_copy(x_ref.at[b, pl.ds(row0, BLK)], inb.at[n % 2], in_sem.at[n % 2]).start()

    def ga_copy(b, i):
        row0 = pl.multiple_of(i * BLK, BLK)
        return pltpu.make_async_copy(gab.at[i % 2], ga_ref.at[b, pl.ds(row0, BLK)], ga_sem.at[i % 2])

    pltpu.make_async_copy(dr_ref.at[0, pl.ds(0, BLK)], inb.at[0], in_sem.at[0]).start()
    pack(w_ref, wq_ref, wk_ref, wv_ref)
    dwq_ref[...] = jnp.zeros_like(dwq_ref)
    dkv_ref[...] = jnp.zeros_like(dkv_ref)
    dwo_ref[...] = jnp.zeros_like(dwo_ref)

    def work(n):
        b, ph = n // (2 * nq), n % (2 * nq)
        row0 = pl.multiple_of((ph % nq) * BLK, BLK)

        @pl.when(n + 1 < count)
        def _():
            fetch(n + 1)

        pltpu.make_async_copy(dr_ref.at[0, pl.ds(0, BLK)], inb.at[n % 2], in_sem.at[n % 2]).wait()

        @pl.when(ph == 0)
        def _():
            dk_s[...] = jnp.zeros_like(dk_s)
            dv_s[...] = jnp.zeros_like(dv_s)

        @pl.when(ph < nq)
        def _():
            dr = inb[n % 2]
            dctx = mm_nt(dr, wo_ref[...]).astype(BF)
            dwo_ref[...] += mm_tn(ctx_ref[b, pl.ds(row0, BLK)], dr)
            q = qkv_ref[b, pl.ds(row0, BLK), :HEAD_DIM]
            k = qkv_ref[b, :, HEAD_DIM:2 * HEAD_DIM]
            v = qkv_ref[b, :, 2 * HEAD_DIM:]
            probs = masked_probs(q, k, sg_ref, b, row0)
            dp = mm_nt(dctx, v)
            ds = (probs * (dp - jnp.sum(dp * probs, axis=-1, keepdims=True)) * scale).astype(BF)
            dv_s[...] += mm_tn(probs.astype(BF), dctx)
            dk_s[...] += mm_tn(ds, q)
            dqkv_s[pl.ds(row0, BLK), :HEAD_DIM] = mm(ds, k).astype(BF)

        @pl.when(ph == nq - 1)
        def _():
            dqkv_s[:, HEAD_DIM:2 * HEAD_DIM] = dk_s[...].astype(BF)
            dqkv_s[:, 2 * HEAD_DIM:] = dv_s[...].astype(BF)

        @pl.when(ph >= nq)
        def _():
            i = ph - nq
            normed, _ = rms_parts(inb[n % 2])
            a = (normed * g_ref[...]).astype(BF)
            blk = dqkv_s[pl.ds(row0, BLK)]
            dw = mm_tn(a, blk)
            dwq_ref[...] += dw[:, :HEAD_DIM]
            dkv_ref[...] += dw[:, HEAD_DIM:]

            @pl.when((b > 0) | (i >= 2))
            def _():
                ga_copy(b, i).wait()

            gab[i % 2] = mm_nt(blk, w_ref[...]).astype(BF)
            ga_copy(b, i).start()

    def end():
        for i in (nq - 2, nq - 1):
            ga_copy(nb - 1, i).wait()

    return work, end, count


def back_scratch(seq, width):
    return [pltpu.VMEM((2, BLK, width), BF), pltpu.VMEM((2, BLK, width), BF), pltpu.VMEM((seq, 3 * HEAD_DIM), BF),
            pltpu.VMEM((seq, HEAD_DIM), F32), pltpu.VMEM((seq, HEAD_DIM), F32), pltpu.VMEM((width, 3 * HEAD_DIM), BF),
            pltpu.SemaphoreType.DMA((2,)), pltpu.SemaphoreType.DMA((2,))]


def finish_kernel(n_copy, *refs):
    ins, outs = refs[:n_copy + 2], refs[n_copy + 2:]
    for n in range(n_copy):
        outs[n][...] = ins[n][...]
    kv, gains = ins[n_copy], ins[n_copy + 1]
    for n in range(2):
        outs[n_copy + n][...] = kv[:, n * HEAD_DIM:(n + 1) * HEAD_DIM]
        outs[n_copy + 2 + n][...] = gains[n:n + 1, :]


def finish_call(by_rows, by_cols, kv, gains):
    steps = 16
    rows = lambda a: pl.BlockSpec((a.shape[0] // steps, a.shape[1]), lambda i: (i, 0))
    cols = lambda a: pl.BlockSpec((a.shape[0], a.shape[1] // steps), lambda i: (0, i))
    half = jax.ShapeDtypeStruct((kv.shape[0], HEAD_DIM), F32)
    gain = jax.ShapeDtypeStruct((1, gains.shape[1]), F32)
    copied = by_rows + by_cols
    specs = [rows(a) for a in by_rows] + [cols(a) for a in by_cols]
    same = pl.BlockSpec(gain.shape, lambda i: (0, 0))
    return pl.pallas_call(
        functools.partial(finish_kernel, len(copied)),
        grid=(steps,),
        in_specs=specs + [rows(kv), pl.BlockSpec(gains.shape, lambda i: (0, 0))],
        out_specs=specs + [rows(half), rows(half), same, same],
        out_shape=[jax.ShapeDtypeStruct(a.shape, a.dtype) for a in copied] + [half, half, gain, gain],
        name='finish',
        compiler_params=pltpu.CompilerParams(vmem_limit_bytes=VMEM_LIMIT),
        cost_estimate=pl.CostEstimate(flops=1_000_000_000, bytes_accessed=60_000_000, transcendentals=0),
    )(*copied, kv, gains)


def mid_kernel(chips, part, x, dy, g_ref, wg, wu, wd, out, p_out, h_own, x_own, dres_own, gpart, dwg, dwu, dwd,
               loc, oth, arr, gat, gat2, dyb, pst, gst, dy_own,
               ld_sem, xs_sem, xr_sem, rs_sem, rr_sem, as_sem, ar_sem, ps_sem, pm_sem, own_sem, dy_sem, po_sem,
               xs2_sem, xr2_sem, rs2_sem, rr2_sem, as2_sem, ar2_sem, ps2_sem, pr2_sem, wo_sem):
    me = lax.axis_index('tp')
    chip = me // 2
    core = me % 2
    mate = chip * 2 + 1 - core
    nxt = (lax.rem(chip + 1, chips) * 2 + core, lax.rem(chip + chips - 1, chips) * 2 + core)
    width = x.shape[-1]
    last = chips - 1

    def remote(src, dst, ssem, rsem, t):
        return pltpu.make_async_remote_copy(src_ref=src, dst_ref=dst, send_sem=ssem, recv_sem=rsem,
                                            device_id={'tp': t}, device_id_type=MESH)

    barrier = pltpu.get_barrier_semaphore()
    for t in (nxt[0], nxt[1], mate):
        pl.semaphore_signal(barrier, inc=1, device_id={'tp': t}, device_id_type=MESH)
    pl.semaphore_wait(barrier, 3)

    def chunk_at(d, s):
        return lax.rem(chip + (s if d == 1 else chips - s), chips)

    def swap(d, s):
        m = chunk_at(d, s)
        return remote(part.at[m * 2 + 1 - core, d], oth.at[m, d], xs_sem, xr_sem.at[m, d], mate)

    def load(d, s):
        m = chunk_at(d, s)
        return pltpu.make_async_copy(part.at[m * 2 + core, d], loc.at[m, d], ld_sem.at[m, d])

    def dy_copy(d, t):
        m = chunk_at(d, t)
        return pltpu.make_async_copy(dy.at[pl.ds(m * 2, 2), d], dyb.at[t % 2, d], dy_sem.at[t % 2, d])

    for s in range(1, chips + 1):
        for d in range(2):
            swap(d, s % chips).start()
            load(d, s % chips).start()
    x_load = pltpu.make_async_copy(x.at[me], x_own, own_sem.at[0])
    dy_load = pltpu.make_async_copy(dy.at[me], dy_own, own_sem.at[1])
    x_load.start()
    dy_load.start()
    for d in range(2):
        dy_copy(d, 0).start()
    for acc in (dwg, dwu, dwd):
        acc[...] = jnp.zeros_like(acc)

    def rs_copy(d, j, s, m, ssem, rsem):
        return remote(loc.at[m, d, j], arr.at[s, d, j], ssem, rsem.at[s, d, j], nxt[d])

    def rs_step(s, first):
        for d in range(2):
            load(d, s + 1).wait()
            swap(d, s + 1).wait_recv()
        for j in range(SUB):
            for d in range(2):
                m = chunk_at(d, s + 1)
                v = loc[m, d, j].astype(F32) + oth[m, d, j].astype(F32)
                if not first:
                    rs_copy(d, j, s - 1, m, rs_sem, rr_sem).wait_recv()
                    v = v + arr[s - 1, d, j].astype(F32)
                loc[m, d, j] = v.astype(BF)
                rs_copy(d, j, s, m, rs_sem, rr_sem).start()

    rs_step(0, True)

    @pl.loop(1, last)
    def _(s):
        rs_step(s, False)

    def ag_copy(d, j, t, m):
        return remote(gat.at[m * 2 + core, d, j], gat.at[m * 2 + core, d, j], as_sem, ar_sem.at[t, d, j], nxt[d])

    def spread(d, j, t, m):
        remote(gat.at[m * 2 + core, d, j], gat.at[m * 2 + core, d, j], ps_sem, pm_sem.at[t], mate).start()

    x_load.wait()
    dy_load.wait()
    for d in range(2):
        load(d, 0).wait()
        swap(d, 0).wait_recv()
    for j in range(SUB):
        for d in range(2):
            rs_copy(d, j, last - 1, chip, rs_sem, rr_sem).wait_recv()
            v = loc[chip, d, j].astype(F32) + oth[chip, d, j].astype(F32) + arr[last - 1, d, j].astype(F32)
            h = (x_own[d, j].astype(F32) + v.astype(BF).astype(F32)).astype(BF)
            h_own[d, j] = h
            normed, _ = rms_parts(h)
            gat[me, d, j] = (normed * g_ref[...]).astype(BF)
            ag_copy(d, j, 0, chip).start()
            spread(d, j, 0, chip)

    def bulk(ref, sem, rsem):
        return remote(ref, ref, sem, rsem, mate)

    bulk(arr, rs_sem, pr2_sem).wait_send()

    def p_copy(d, t):
        m = chunk_at(d, t)
        return pltpu.make_async_copy(pst.at[t % 2, d], p_out.at[pl.ds(m * 2, 2), d], po_sem.at[t % 2, d])

    def swap2(d, t):
        m = chunk_at(d, t)
        return remote(gst.at[t % 2, d, 1 - core], oth.at[m, d], xs2_sem.at[t % 2, d], xr2_sem.at[m, d], mate)

    def rs2_step(t, first):
        slot = t % 2
        for d in range(2):
            swap2(d, t).wait_recv()
        for j in range(SUB):
            for d in range(2):
                m = chunk_at(d, t)
                v = gst[slot, d, core, j].astype(F32) + oth[m, d, j].astype(F32)
                if not first:
                    rs_copy(d, j, t - 2, m, rs2_sem, rr2_sem).wait_recv()
                    v = v + arr[t - 2, d, j].astype(F32)
                loc[m, d, j] = v.astype(BF)
                rs_copy(d, j, t - 1, m, rs2_sem, rr2_sem).start()

    def collect(t, onward):
        for j in range(SUB):
            for d in range(2):
                m = chunk_at(d, t)
                ag_copy(d, j, t - 1, m).wait_recv()
                if onward:
                    ag_copy(d, j, t, m).start()
                spread(d, j, t, m)

    step = width // 4

    @pl.loop(0, chips)
    def _(t):
        slot = t % 2
        a = chunk_at(0, t)
        b = chunk_at(1, t)

        @pl.when((t > 0) & (t < last))
        def _():
            collect(t, True)

        @pl.when(t == last)
        def _():
            collect(t, False)

        @pl.when(t < last)
        def _():
            for d in range(2):
                dy_copy(d, t + 1).start()

        @pl.when(t >= 2)
        def _():
            for d in range(2):
                p_copy(d, t - 2).wait()
                swap2(d, t - 2).wait_send()

        for d in range(2):
            dy_copy(d, t).wait()
        bulk(gat.at[0], ps_sem, pm_sem.at[t]).wait_recv()

        rows = 4 * SUB * ROWS
        mb = jnp.concatenate([gat[pl.ds(a * 2, 2), 0].reshape(rows // 2, width), gat[pl.ds(b * 2, 2), 1].reshape(rows // 2, width)], axis=0)
        dyv = dyb[slot].reshape(rows, width)
        gate = mm_nt(mb, wg[...])
        upper = mm_nt(mb, wu[...])
        dact = mm_nt(dyv, wd[...])
        sig = jax.nn.sigmoid(gate)
        act = (gate * sig * upper).astype(BF)
        dgate = (dact * upper * sig * (1.0 + gate * (1.0 - sig))).astype(BF)
        dupper = (dact * gate * sig).astype(BF)
        for n in range(4):
            cs = slice(n * step, (n + 1) * step)
            gst[slot, :, :, :, :, cs] = (mm(dgate, wg[:, cs]) + mm(dupper, wu[:, cs])).astype(BF).reshape(2, 2, SUB, ROWS, step)
        for d in range(2):
            swap2(d, t).start()
        for n in range(4):
            cs = slice(n * step, (n + 1) * step)
            pst[slot, :, :, :, :, cs] = mm(act, wd[:, cs]).astype(BF).reshape(2, 2, SUB, ROWS, step)
            dwd[:, cs] += mm_tn(act, dyv[:, cs])
            dwg[:, cs] += mm_tn(dgate, mb[:, cs])
            dwu[:, cs] += mm_tn(dupper, mb[:, cs])
        for d in range(2):
            p_copy(d, t).start()

        @pl.when(t == 0)
        def _():
            for d in range(2):
                loc[chip, d] = gst[0, d, core]

        @pl.when(t == 1)
        def _():
            rs2_step(t, True)

        @pl.when(t > 1)
        def _():
            rs2_step(t, False)

    def ag2_copy(d, j, t, m):
        return remote(gat2.at[m, d, j], gat2.at[m, d, j], as2_sem, ar2_sem.at[t, d, j], nxt[d])

    def spread2(d, j, m):
        remote(gat2.at[m, d, j], out.at[m * 2 + core, d, j], ps2_sem, pr2_sem, mate).start()
        pltpu.make_async_copy(gat2.at[m, d, j], out.at[m * 2 + core, d, j], wo_sem).start()

    for d in range(2):
        swap2(d, 0).wait_recv()
    total = jnp.zeros((1, width), F32)
    for j in range(SUB):
        for d in range(2):
            rs_copy(d, j, last - 1, chip, rs2_sem, rr2_sem).wait_recv()
            v = loc[chip, d, j].astype(F32) + oth[chip, d, j].astype(F32) + arr[last - 1, d, j].astype(F32)
            v = v.astype(BF).astype(F32)
            normed, inv = rms_parts(h_own[d, j])
            total = total + jnp.sum(v * normed, axis=0, keepdims=True)
            grad = dy_own[d, j].astype(F32) + rms_back(v, normed, inv, g_ref[...])
            dres_own[d, j] = grad
            gat2[chip, d, j] = grad.astype(BF)
            ag2_copy(d, j, 0, chip).start()
            spread2(d, j, chip)
    gpart[...] = total

    def ag2_step(t, onward):
        for j in range(SUB):
            for d in range(2):
                m = chunk_at(d, t)
                ag2_copy(d, j, t - 1, m).wait_recv()
                if onward:
                    ag2_copy(d, j, t, m).start()
                spread2(d, j, m)

    @pl.loop(1, last)
    def _(t):
        ag2_step(t, True)

    ag2_step(last, False)

    bulk(gat2, ps2_sem, pr2_sem).wait_recv()
    for sem in (xs_sem, ps_sem, ps2_sem):
        bulk(oth, sem, pr2_sem).wait_send()
    for sem in (as_sem, rs2_sem, as2_sem):
        bulk(arr, sem, pr2_sem).wait_send()
    for t in (chips - 2, chips - 1):
        for d in range(2):
            p_copy(d, t).wait()
            swap2(d, t).wait_send()
    pltpu.make_async_copy(gat2, gat2, wo_sem).wait()


def mid_call(part, x, dy, gain, w_gate, w_up, w_down, chips, cid):
    tokens, width = part.shape
    ff = w_down.shape[0]
    shape = (chips * 2, 2, SUB, ROWS, width)
    half = (chips, 2, SUB, ROWS, width)
    arrive = (chips - 1, 2, SUB, ROWS, width)
    piece = (2, SUB, ROWS, width)
    pair = (2, 2, 2, SUB, ROWS, width)
    vm = pl.BlockSpec(memory_space=pltpu.VMEM)
    anyspec = pl.BlockSpec(memory_space=pl.ANY)
    dma = pltpu.SemaphoreType.DMA
    steps = dma((chips - 1, 2, SUB))
    vmb = lambda shp: pltpu.VMEM(shp, BF)
    grad = jax.ShapeDtypeStruct((ff, width), F32)
    res = pl.pallas_call(
        functools.partial(mid_kernel, chips),
        out_shape=[jax.ShapeDtypeStruct(shape, BF), jax.ShapeDtypeStruct(shape, BF), jax.ShapeDtypeStruct(piece, BF),
                   jax.ShapeDtypeStruct(piece, BF), jax.ShapeDtypeStruct(piece, F32), jax.ShapeDtypeStruct((1, width), F32),
                   grad, grad, grad],
        in_specs=[anyspec] * 3 + [vm] * 4,
        out_specs=[anyspec] * 2 + [vm] * 7,
        scratch_shapes=[
            vmb(half), vmb(half), vmb(arrive), vmb(shape), vmb(half), vmb(pair), vmb(pair), vmb(pair), vmb(piece),
            dma((chips, 2)), dma, dma((chips, 2)), dma, steps, dma, steps, dma, dma((chips,)), dma((2,)), dma((2, 2)), dma((2, 2)),
            dma((2, 2)), dma((chips, 2)), dma, steps, dma, steps, dma, dma, dma],
        name='middle',
        compiler_params=pltpu.CompilerParams(collective_id=cid, has_side_effects=True, vmem_limit_bytes=67_000_000),
        cost_estimate=pl.CostEstimate(flops=120_000_000_000, bytes_accessed=40 * tokens * width, transcendentals=0),
    )(part.reshape(shape), x.reshape(shape), dy.reshape(shape), gain, w_gate, w_up, w_down)
    return (res[0].reshape(tokens, width), res[1].reshape(tokens, width)) + tuple(res[2:])


def solution(mesh):
    tp_size = mesh.shape['tp']
    chips = tp_size // 2

    def device_step(hidden, seg_ids, grad_out, gain_attn, gain_mlp, w_q, w_k, w_v, w_o, w_gate, w_up, w_down):
        nb, seq, width = hidden.shape
        tokens = nb * seq
        own = tokens // tp_size
        g1 = gain_attn[None, :]
        g2 = gain_mlp[None, :]
        o_part, qkv, ctx = front_call(hidden, seg_ids, g1, w_q, w_k, w_v, w_o)
        dres, p_part, h_own, x_own, dres_own, g2_part, d_gate, d_up, d_down = mid_call(
            o_part.reshape(tokens, width), hidden, grad_out, g2, w_gate.T, w_up.T, w_down, chips, 1)
        grad_q = jax.ShapeDtypeStruct((width, HEAD_DIM), F32)
        grad_kv = jax.ShapeDtypeStruct((width, 2 * HEAD_DIM), F32)
        grad_o = jax.ShapeDtypeStruct((HEAD_DIM, width), F32)
        y_out, ga_part, d_q, d_kv, d_o = ring_call(
            p_part, [h_own, dres.reshape(nb, seq, width), hidden, seg_ids, g1, w_q, w_k, w_v, w_o, qkv, ctx],
            [jax.ShapeDtypeStruct((nb, seq, width), BF), grad_q, grad_kv, grad_o], AddTail, chips, 4,
            task=back_task, in_any=(1, 2), out_any=(0,), extra=back_scratch(seq, width))
        kv_shape = (tp_size, 2, own // 2, 2 * HEAD_DIM)
        dx, gains, d_kv = ring_call(ga_part.reshape(tokens, width), [x_own, dres_own, g1, g1, g2_part, d_kv.reshape(kv_shape)],
                                    [jax.ShapeDtypeStruct((2, width), F32), jax.ShapeDtypeStruct(kv_shape, F32)], AttnTail, chips, 3, True)
        y_out, dx, d_q, d_gate, d_up, d_down, d_o, d_k, d_v, d_g2, d_g1 = finish_call(
            [y_out, dx, d_q], [d_gate, d_up, d_down, d_o], d_kv.reshape(width, 2 * HEAD_DIM), gains)
        return (y_out.reshape(nb, seq, width), dx.reshape(nb, seq, width), d_g1[0], d_g2[0], d_q, d_k, d_v,
                d_o, d_gate.T, d_up.T, d_down)

    spec_act = P('data', None, None)
    spec_rows = P('data', None)
    spec_gain = P(None)
    spec_cols = P(None, 'tp')
    spec_tprows = P('tp', None)
    spec_whole = P(None, None)
    spec_stack = P(('data', 'tp'), None)
    in_specs = (spec_act, spec_rows, spec_act, spec_gain, spec_gain, spec_cols, spec_whole, spec_whole, spec_tprows, spec_cols, spec_cols, spec_tprows)
    out_specs = (spec_act, spec_act, P('data'), P('data'), P('data', 'tp'), spec_rows, spec_rows, spec_stack, P('data', 'tp'), P('data', 'tp'), spec_stack)
    return jax.shard_map(device_step, mesh=mesh, in_specs=in_specs, out_specs=out_specs, check_vma=False)
```

```python
import functools
import jax
import jax.numpy as jnp
from jax import lax
from jax.experimental import pallas as pl
from jax.experimental.pallas import tpu as pltpu
from jax.sharding import PartitionSpec as P

HEAD_DIM = 128
EPS = 1e-5
SUB = 4
ROWS = 16
BLK = 256
BF = jnp.bfloat16
F32 = jnp.float32
MESH = pl.DeviceIdType.MESH
VMEM_LIMIT = 60 * 1024 * 1024


def mm(a, b):
    return lax.dot_general(a, b, (((1,), (0,)), ((), ())), preferred_element_type=F32)


def mm_nt(a, b):
    return lax.dot_general(a, b, (((1,), (1,)), ((), ())), preferred_element_type=F32)


def mm_tn(a, b):
    return lax.dot_general(a, b, (((0,), (0,)), ((), ())), preferred_element_type=F32)


def rms_parts(x_in):
    x_float = x_in.astype(F32)
    inv = lax.rsqrt(jnp.mean(x_float * x_float, axis=-1, keepdims=True) + EPS)
    return x_float * inv, inv


def rms_back(grad, normed, inv, gain):
    scaled = grad * gain
    return inv * (scaled - normed * jnp.mean(scaled * normed, axis=-1, keepdims=True))


def ring_kernel(chips, n_in, n_out, epilogue, with_gain, task, part, *refs):
    ins = refs[:n_in]
    out = refs[n_in]
    outs = refs[n_in + 1:n_in + 1 + n_out]
    scratch = refs[n_in + 1 + n_out:]
    (loc, oth, arr, gat, ld_sem, xs_sem, xr_sem, rs_sem, rr_sem, as_sem, ar_sem, ps_sem, pr_sem, wo_sem) = scratch[:14]
    me = lax.axis_index('tp')
    chip = me // 2
    core = me % 2
    mate = chip * 2 + 1 - core
    nxt = (lax.rem(chip + 1, chips) * 2 + core, lax.rem(chip + chips - 1, chips) * 2 + core)

    def dev(t):
        return {'tp': t}

    barrier = pltpu.get_barrier_semaphore()
    for t in (nxt[0], nxt[1], mate):
        pl.semaphore_signal(barrier, inc=1, device_id=dev(t), device_id_type=MESH)
    pl.semaphore_wait(barrier, 3)

    def chunk_at(d, s):
        off = s if d == 1 else chips - s
        return lax.rem(chip + off, chips)

    def swap(d, s):
        m = chunk_at(d, s)
        return pltpu.make_async_remote_copy(
            src_ref=part.at[m * 2 + 1 - core, d], dst_ref=oth.at[m, d], send_sem=xs_sem,
            recv_sem=xr_sem.at[m, d], device_id=dev(mate), device_id_type=MESH)

    def load(d, s):
        m = chunk_at(d, s)
        return pltpu.make_async_copy(part.at[m * 2 + core, d], loc.at[m, d], ld_sem.at[m, d])

    if with_gain:
        (gacc, gbuf, gmate, gs_sem, gr_sem, gms_sem, gmr_sem, kacc, koth, karr, kxs, kxr, krs, krr, kas, kar, kps, kpr) = scratch[14:]
        kin, kout = ins[5], outs[1]

        def kswap(d, s):
            m = chunk_at(d, s)
            return pltpu.make_async_remote_copy(
                src_ref=kin.at[m * 2 + 1 - core, d], dst_ref=koth.at[m, d], send_sem=kxs,
                recv_sem=kxr.at[m, d], device_id=dev(mate), device_id_type=MESH)

        def krs_copy(d, s, m):
            return pltpu.make_async_remote_copy(
                src_ref=kacc.at[m, d], dst_ref=karr.at[s, d], send_sem=krs,
                recv_sem=krr.at[s, d], device_id=dev(nxt[d]), device_id_type=MESH)

        def kag_copy(d, t, m):
            return pltpu.make_async_remote_copy(
                src_ref=kout.at[m * 2 + core, d], dst_ref=kout.at[m * 2 + core, d], send_sem=kas,
                recv_sem=kar.at[t, d], device_id=dev(nxt[d]), device_id_type=MESH)

        def kspread(d, m):
            pltpu.make_async_remote_copy(
                src_ref=kout.at[m * 2 + core, d], dst_ref=kout.at[m * 2 + core, d], send_sem=kps,
                recv_sem=kpr, device_id=dev(mate), device_id_type=MESH).start()

    for s in range(1, chips + 1):
        for d in range(2):
            swap(d, s % chips).start()
            load(d, s % chips).start()
            if with_gain:
                kswap(d, s % chips).start()

    def rs_copy(d, j, s, m):
        return pltpu.make_async_remote_copy(
            src_ref=loc.at[m, d, j], dst_ref=arr.at[s, d, j], send_sem=rs_sem,
            recv_sem=rr_sem.at[s, d, j], device_id=dev(nxt[d]), device_id_type=MESH)

    def ready(d, s):
        load(d, s).wait()
        swap(d, s).wait_recv()

    def rs_step(s, first):
        for d in range(2):
            ready(d, s + 1)
        for j in range(SUB):
            for d in range(2):
                m = chunk_at(d, s + 1)
                v = loc[m, d, j].astype(F32) + oth[m, d, j].astype(F32)
                if not first:
                    rs_copy(d, j, s - 1, m).wait_recv()
                    v = v + arr[s - 1, d, j].astype(F32)
                loc[m, d, j] = v.astype(BF)
                rs_copy(d, j, s, m).start()
        if with_gain:
            for d in range(2):
                m = chunk_at(d, s + 1)
                kswap(d, s + 1).wait_recv()
                kv = kin[m * 2 + core, d] + koth[m, d]
                if not first:
                    krs_copy(d, s - 1, m).wait_recv()
                    kv = kv + karr[s - 1, d]
                kacc[m, d] = kv
                krs_copy(d, s, m).start()

    rs_step(0, True)

    if task:
        work, work_end, work_count = task(ins, outs, scratch[14:])

    def work_share(n):
        if task:
            lead = chips
            rest = work_count - lead
            span = chips - 2
            if isinstance(n, int):
                work(jnp.int32(n))
            else:
                late = jnp.maximum(n - lead, 0)
                lo = jnp.where(n < lead, n, lead + late * rest // span)
                hi = jnp.where(n < lead, n + 1, lead + (late + 1) * rest // span)
                pl.loop(lo, hi)(work)

    work_share(0)

    @pl.loop(1, chips - 1)
    def _(s):
        rs_step(s, False)
        work_share(s)

    def ag_copy(d, j, t, m):
        return pltpu.make_async_remote_copy(
            src_ref=gat.at[m, d, j], dst_ref=gat.at[m, d, j], send_sem=as_sem,
            recv_sem=ar_sem.at[t, d, j], device_id=dev(nxt[d]), device_id_type=MESH)

    def spread(d, j, m):
        pltpu.make_async_remote_copy(
            src_ref=gat.at[m, d, j], dst_ref=out.at[m * 2 + core, d, j], send_sem=ps_sem,
            recv_sem=pr_sem, device_id=dev(mate), device_id_type=MESH).start()
        pltpu.make_async_copy(gat.at[m, d, j], out.at[m * 2 + core, d, j], wo_sem).start()

    for d in range(2):
        ready(d, 0)
    state = epilogue.begin(ins, outs)
    for j in range(SUB):
        for d in range(2):
            rs_copy(d, j, chips - 2, chip).wait_recv()
            v = loc[chip, d, j].astype(F32) + oth[chip, d, j].astype(F32) + arr[chips - 2, d, j].astype(F32)
            res, state = epilogue.piece(v.astype(BF).astype(F32), d, j, ins, outs, state)
            gat[chip, d, j] = res
            ag_copy(d, j, 0, chip).start()
            spread(d, j, chip)
    epilogue.end(outs, state)

    work_share(chips - 1)

    if with_gain:
        for d in range(2):
            kswap(d, 0).wait_recv()
            krs_copy(d, chips - 2, chip).wait_recv()
            kout[chip * 2 + core, d] = kin[chip * 2 + core, d] + koth[chip, d] + karr[chips - 2, d]
            kag_copy(d, 0, chip).start()
            kspread(d, chip)

        def gain_copy(t, src):
            return pltpu.make_async_remote_copy(
                src_ref=src, dst_ref=gbuf.at[t], send_sem=gs_sem.at[t],
                recv_sem=gr_sem.at[t], device_id=dev(nxt[0]), device_id_type=MESH)

        gacc[0:1] = ins[4][...]
        gacc[1:2] = state
        gain_copy(0, gacc).start()

    def ag_step(t, last):
        for j in range(SUB):
            for d in range(2):
                m = chunk_at(d, t)
                ag_copy(d, j, t - 1, m).wait_recv()
                if not last:
                    ag_copy(d, j, t, m).start()
                spread(d, j, m)
        if with_gain:
            for d in range(2):
                m = chunk_at(d, t)
                kag_copy(d, t - 1, m).wait_recv()
                if not last:
                    kag_copy(d, t, m).start()
                kspread(d, m)
            gain_copy(t - 1, gacc).wait_recv()
            if not last:
                gain_copy(t, gbuf.at[t - 1]).start()

    @pl.loop(1, chips - 1)
    def _(t):
        ag_step(t, False)
        work_share(chips - 1 + t)

    ag_step(chips - 1, True)
    if task:
        work_end()

    if with_gain:
        tot = gacc[...]
        for t in range(chips - 1):
            tot = tot + gbuf[t]
            gain_copy(t, gacc).wait_send()
        outs[0][...] = tot
        mate_copy = pltpu.make_async_remote_copy(
            src_ref=outs[0], dst_ref=gmate, send_sem=gms_sem, recv_sem=gmr_sem,
            device_id=dev(mate), device_id_type=MESH)
        mate_copy.start()
        mate_copy.wait()
        outs[0][...] = tot + gmate[...]

    def bulk(ref, sem, rsem):
        return pltpu.make_async_remote_copy(
            src_ref=ref, dst_ref=ref, send_sem=sem, recv_sem=rsem, device_id=dev(mate), device_id_type=MESH)

    if with_gain:
        bulk(koth, kps, kpr).wait_recv()
        bulk(koth, kxs, kpr).wait_send()
        bulk(karr, krs, kpr).wait_send()
        bulk(karr, kas, kpr).wait_send()
        bulk(koth, kps, kpr).wait_send()
    bulk(gat, ps_sem, pr_sem).wait_recv()
    bulk(oth, xs_sem, pr_sem).wait_send()
    bulk(arr, rs_sem, pr_sem).wait_send()
    bulk(arr, as_sem, pr_sem).wait_send()
    bulk(gat, ps_sem, pr_sem).wait_send()
    pltpu.make_async_copy(gat, gat, wo_sem).wait()


class AddTail:
    @staticmethod
    def begin(ins, outs):
        return None

    @staticmethod
    def piece(v, d, j, ins, outs, state):
        return (ins[0][d, j].astype(F32) + v).astype(BF), state

    @staticmethod
    def end(outs, state):
        pass


class AttnTail:
    @staticmethod
    def begin(ins, outs):
        return jnp.zeros(ins[2].shape, F32)

    @staticmethod
    def piece(v, d, j, ins, outs, state):
        normed, inv = rms_parts(ins[0][d, j])
        state = state + jnp.sum(v * normed, axis=0, keepdims=True)
        grad = ins[1][d, j] + rms_back(v, normed, inv, ins[2][...])
        return grad.astype(BF), state

    @staticmethod
    def end(outs, state):
        pass


def ring_call(part, ins, out_shapes, epilogue, chips, cid, with_gain=False, task=None, in_any=(), out_any=(), extra=()):
    tokens, width = part.shape
    shape = (chips * 2, 2, SUB, ROWS, width)
    half = (chips, 2, SUB, ROWS, width)
    arrive = (chips - 1, 2, SUB, ROWS, width)
    vm = pl.BlockSpec(memory_space=pltpu.VMEM)
    anyspec = pl.BlockSpec(memory_space=pl.ANY)
    dma = pltpu.SemaphoreType.DMA
    scratch = [
        pltpu.VMEM(half, BF), pltpu.VMEM(half, BF), pltpu.VMEM(arrive, BF), pltpu.VMEM(half, BF),
        dma((chips, 2)), dma, dma((chips, 2)), dma, dma((chips - 1, 2, SUB)), dma,
        dma((chips - 1, 2, SUB)), dma, dma, dma]
    if with_gain:
        scratch += [pltpu.VMEM((2, width), F32), pltpu.VMEM((chips - 1, 2, width), F32), pltpu.VMEM((2, width), F32),
                    dma((chips - 1,)), dma((chips - 1,)), dma, dma]
        kshape = ins[5].shape[1:]
        scratch += [pltpu.VMEM((chips,) + kshape, F32), pltpu.VMEM((chips,) + kshape, F32), pltpu.VMEM((chips - 1,) + kshape, F32),
                    dma, dma((chips, 2)), dma, dma((chips - 1, 2)), dma, dma((chips - 1, 2)), dma, dma]
    scratch += list(extra)
    n_in, n_out = len(ins), len(out_shapes)

    def body(*refs):
        ring_kernel(chips, n_in, n_out, epilogue, with_gain, task, *refs)

    res = pl.pallas_call(
        body,
        out_shape=[jax.ShapeDtypeStruct(shape, BF)] + out_shapes,
        in_specs=[anyspec] + [anyspec if n in in_any else vm for n in range(n_in)],
        out_specs=[anyspec] + [anyspec if n in out_any else vm for n in range(n_out)],
        scratch_shapes=scratch,
        name='ring_%d' % cid,
        compiler_params=pltpu.CompilerParams(collective_id=cid, has_side_effects=True, vmem_limit_bytes=VMEM_LIMIT),
        cost_estimate=pl.CostEstimate(flops=80_000_000_000, bytes_accessed=4 * tokens * width, transcendentals=0),
    )(part.reshape(shape), *ins)
    return (res[0].reshape(tokens, width),) + tuple(res[1:])


def seg_column(seg_ref, b, row0, n):
    own = seg_ref[pl.ds(b, 1), pl.ds(row0, n)].astype(F32)
    return jnp.transpose(jnp.broadcast_to(own, (128, n)))[:, :1]


def masked_probs(q, k, seg_q, seg_k, row0, split=0):
    s = mm_nt(q, k) * HEAD_DIM ** -0.5
    local = lax.broadcasted_iota(jnp.int32, s.shape, 0)
    rows = row0 + local
    if split:
        rows = rows + jnp.where(local >= q.shape[0] // 2, split, 0)
    cols = lax.broadcasted_iota(jnp.int32, s.shape, 1)
    s = jnp.where((rows >= cols) & (seg_q == seg_k), s, -1e30)
    e = jnp.exp(s - jnp.max(s, axis=-1, keepdims=True))
    return e * (1.0 / jnp.sum(e, axis=-1, keepdims=True))


def pack(w_ref, wq_ref, wk_ref, wv_ref):
    for n, ref in enumerate((wq_ref, wk_ref, wv_ref)):
        w_ref[:, n * HEAD_DIM:(n + 1) * HEAD_DIM] = ref[...]


def front_kernel(x_ref, g_ref, wq_ref, wk_ref, wv_ref, qkv_ref, w_ref):
    @pl.when(pl.program_id(0) == 0)
    def _():
        pack(w_ref, wq_ref, wk_ref, wv_ref)

    normed, _ = rms_parts(x_ref[...])
    qkv_ref[...] = mm((normed * g_ref[...]).astype(BF), w_ref[...]).astype(BF)


def front_call(x, gain, w_q, w_k, w_v):
    tokens, width = x.shape
    e3 = 3 * HEAD_DIM
    rowblk = lambda n: pl.BlockSpec((BLK, n), lambda i: (i, 0))
    whole = lambda arr: pl.BlockSpec(arr.shape, lambda i: (0, 0))
    return pl.pallas_call(
        front_kernel,
        grid=(tokens // BLK,),
        in_specs=[rowblk(width), whole(gain), whole(w_q), whole(w_k), whole(w_v)],
        out_specs=rowblk(e3),
        out_shape=jax.ShapeDtypeStruct((tokens, e3), BF),
        scratch_shapes=[pltpu.VMEM((width, e3), BF)],
        name='front',
        compiler_params=pltpu.CompilerParams(vmem_limit_bytes=VMEM_LIMIT),
        cost_estimate=pl.CostEstimate(flops=4_000_000_000, bytes_accessed=12_000_000, transcendentals=0),
    )(x, gain, w_q, w_k, w_v)


def back_task(ins, outs, scratch):
    dr_ref, x_ref, sg_ref, g_ref, wq_ref, wk_ref, wv_ref, wo_ref, qkv_ref = ins[1:]
    ga_ref, dwq_ref, dkv_ref, dwo_ref = outs
    inb, gab, dqkv_s, dk_s, dv_s, w_ref, in_sem, ga_sem = scratch
    nb, seq, width = dr_ref.shape
    nq = seq // BLK
    count = nb * 2 * nq
    scale = HEAD_DIM ** -0.5

    def fetch(n):
        b, ph = n // (2 * nq), n % (2 * nq)
        row0 = pl.multiple_of((ph % nq) * BLK, BLK)

        @pl.when(ph < nq)
        def _():
            pltpu.make_async_copy(dr_ref.at[b, pl.ds(row0, BLK)], inb.at[n % 2], in_sem.at[n % 2]).start()

        @pl.when(ph >= nq)
        def _():
            pltpu.make_async_copy(x_ref.at[b, pl.ds(row0, BLK)], inb.at[n % 2], in_sem.at[n % 2]).start()

    def ga_copy(b, i):
        row0 = pl.multiple_of(i * BLK, BLK)
        return pltpu.make_async_copy(gab.at[i % 2], ga_ref.at[b, pl.ds(row0, BLK)], ga_sem.at[i % 2])

    pltpu.make_async_copy(dr_ref.at[0, pl.ds(0, BLK)], inb.at[0], in_sem.at[0]).start()
    pack(w_ref, wq_ref, wk_ref, wv_ref)
    dwq_ref[...] = jnp.zeros_like(dwq_ref)
    dkv_ref[...] = jnp.zeros_like(dkv_ref)
    dwo_ref[...] = jnp.zeros_like(dwo_ref)

    def work(n):
        b, ph = n // (2 * nq), n % (2 * nq)
        row0 = pl.multiple_of((ph % nq) * BLK, BLK)

        @pl.when(n + 1 < count)
        def _():
            fetch(n + 1)

        pltpu.make_async_copy(dr_ref.at[0, pl.ds(0, BLK)], inb.at[n % 2], in_sem.at[n % 2]).wait()

        @pl.when(ph == 0)
        def _():
            dk_s[...] = jnp.zeros_like(dk_s)
            dv_s[...] = jnp.zeros_like(dv_s)

        @pl.when(ph < nq)
        def _():
            dr = inb[n % 2]
            dctx = mm_nt(dr, wo_ref[...]).astype(BF)
            q = qkv_ref[b, pl.ds(row0, BLK), :HEAD_DIM]
            k = qkv_ref[b, :, HEAD_DIM:2 * HEAD_DIM]
            v = qkv_ref[b, :, 2 * HEAD_DIM:]
            probs = masked_probs(q, k, seg_column(sg_ref, b, row0, BLK), sg_ref[pl.ds(b, 1), :].astype(F32), row0)
            probs_b = probs.astype(BF)
            dwo_ref[...] += mm_tn(mm(probs_b, v).astype(BF), dr)
            dp = mm_nt(dctx, v)
            ds = (probs * (dp - jnp.sum(dp * probs, axis=-1, keepdims=True)) * scale).astype(BF)
            dv_s[...] += mm_tn(probs_b, dctx)
            dk_s[...] += mm_tn(ds, q)
            dqkv_s[pl.ds(row0, BLK), :HEAD_DIM] = mm(ds, k).astype(BF)

        @pl.when(ph == nq - 1)
        def _():
            dqkv_s[:, HEAD_DIM:2 * HEAD_DIM] = dk_s[...].astype(BF)
            dqkv_s[:, 2 * HEAD_DIM:] = dv_s[...].astype(BF)

        @pl.when(ph >= nq)
        def _():
            i = ph - nq
            normed, _ = rms_parts(inb[n % 2])
            a = (normed * g_ref[...]).astype(BF)
            blk = dqkv_s[pl.ds(row0, BLK)]
            dw = mm_tn(a, blk)
            dwq_ref[...] += dw[:, :HEAD_DIM]
            dkv_ref[...] += dw[:, HEAD_DIM:]

            @pl.when((b > 0) | (i >= 2))
            def _():
                ga_copy(b, i).wait()

            gab[i % 2] = mm_nt(blk, w_ref[...]).astype(BF)
            ga_copy(b, i).start()

    def end():
        for i in (nq - 2, nq - 1):
            ga_copy(nb - 1, i).wait()

    return work, end, count


def back_scratch(seq, width):
    return [pltpu.VMEM((2, BLK, width), BF), pltpu.VMEM((2, BLK, width), BF), pltpu.VMEM((seq, 3 * HEAD_DIM), BF),
            pltpu.VMEM((seq, HEAD_DIM), F32), pltpu.VMEM((seq, HEAD_DIM), F32), pltpu.VMEM((width, 3 * HEAD_DIM), BF),
            pltpu.SemaphoreType.DMA((2,)), pltpu.SemaphoreType.DMA((2,))]


def finish_kernel(n_copy, *refs):
    ins, outs = refs[:n_copy + 2], refs[n_copy + 2:]
    for n in range(n_copy):
        outs[n][...] = ins[n][...]
    kv, gains = ins[n_copy], ins[n_copy + 1]
    for n in range(2):
        outs[n_copy + n][...] = kv[:, n * HEAD_DIM:(n + 1) * HEAD_DIM]
        outs[n_copy + 2 + n][...] = gains[n:n + 1, :]


def finish_call(by_rows, by_parts, kv, gains):
    steps = 16
    rows = lambda a: pl.BlockSpec((a.shape[0] // steps, a.shape[1]), lambda i: (i, 0))
    def parts(a):
        size = next(n for n in range(8, a.shape[0] + 1, 8) if a.shape[0] % n == 0 and a.shape[0] // n <= steps)
        top = a.shape[0] // size - 1
        return pl.BlockSpec((size, a.shape[1]), lambda i: (jnp.minimum(i, top), 0))

    half = jax.ShapeDtypeStruct((kv.shape[0], HEAD_DIM), F32)
    gain = jax.ShapeDtypeStruct((1, gains.shape[1]), F32)
    copied = by_rows + by_parts
    specs = [rows(a) for a in by_rows] + [parts(a) for a in by_parts]
    same = pl.BlockSpec(gain.shape, lambda i: (0, 0))
    return pl.pallas_call(
        functools.partial(finish_kernel, len(copied)),
        grid=(steps,),
        in_specs=specs + [rows(kv), pl.BlockSpec(gains.shape, lambda i: (0, 0))],
        out_specs=specs + [rows(half), rows(half), same, same],
        out_shape=[jax.ShapeDtypeStruct(a.shape, a.dtype) for a in copied] + [half, half, gain, gain],
        name='finish',
        compiler_params=pltpu.CompilerParams(vmem_limit_bytes=VMEM_LIMIT),
        cost_estimate=pl.CostEstimate(flops=1_000_000_000, bytes_accessed=60_000_000, transcendentals=0),
    )(*copied, kv, gains)


def mid_kernel(chips, x, dy, g_ref, seg, qkv, wo, wg, wu, wd, out, p_out, h_own, x_own, dres_own, gpart, dwg, dwu, dwd,
               loc, oth, arr, gat, gat2, dyb, pst, gst, dy_own,
               xs_sem, xr_sem, rs_sem, rr_sem, as_sem, ar_sem, ps_sem, pm_sem, own_sem, dy_sem, po_sem,
               xs2_sem, xr2_sem, rs2_sem, rr2_sem, as2_sem, ar2_sem, ps2_sem, pr2_sem, wo_sem):
    me = lax.axis_index('tp')
    chip = me // 2
    core = me % 2
    mate = chip * 2 + 1 - core
    nxt = (lax.rem(chip + 1, chips) * 2 + core, lax.rem(chip + chips - 1, chips) * 2 + core)
    width = x.shape[-1]
    last = chips - 1

    def remote(src, dst, ssem, rsem, t):
        return pltpu.make_async_remote_copy(src_ref=src, dst_ref=dst, send_sem=ssem, recv_sem=rsem,
                                            device_id={'tp': t}, device_id_type=MESH)

    barrier = pltpu.get_barrier_semaphore()
    for t in (nxt[0], nxt[1], mate):
        pl.semaphore_signal(barrier, inc=1, device_id={'tp': t}, device_id_type=MESH)
    pl.semaphore_wait(barrier, 3)

    def chunk_at(d, s):
        return lax.rem(chip + (s if d == 1 else chips - s), chips)

    def swap(d, t):
        m = chunk_at(d, t)
        return remote(gst.at[t % 2, d, 1 - core], oth.at[m, d], xs_sem.at[t % 2, d], xr_sem.at[m, d], mate)

    def dy_copy(d, t):
        m = chunk_at(d, t)
        return pltpu.make_async_copy(dy.at[pl.ds(m * 2, 2), d], dyb.at[t % 2, d], dy_sem.at[t % 2, d])

    x_load = pltpu.make_async_copy(x.at[me], x_own, own_sem.at[0])
    dy_load = pltpu.make_async_copy(dy.at[me], dy_own, own_sem.at[1])
    x_load.start()
    dy_load.start()
    for d in range(2):
        dy_copy(d, 0).start()
    for acc in (dwg, dwu, dwd):
        acc[...] = jnp.zeros_like(acc)

    def rs_copy(d, j, s, m, ssem, rsem):
        return remote(loc.at[m, d, j], arr.at[s, d, j], ssem, rsem.at[s, d, j], nxt[d])

    own = SUB * ROWS
    group = chips // qkv.shape[0]

    def attend(t):
        for d in range(2):
            m = chunk_at(d, t)
            b = m // group
            base = pl.multiple_of((m % group) * 4 * own, 4 * own)
            first = pl.multiple_of(base + d * own, own)
            again = pl.multiple_of(base + (2 + d) * own, own)
            q = jnp.concatenate([qkv[b, pl.ds(first, own), :HEAD_DIM], qkv[b, pl.ds(again, own), :HEAD_DIM]], axis=0)
            col = seg_column(seg, b, base, 4 * own)
            seg_q = jnp.concatenate([col[d * own:(d + 1) * own], col[(2 + d) * own:(3 + d) * own]], axis=0)
            probs = masked_probs(q, qkv[b, :, HEAD_DIM:2 * HEAD_DIM], seg_q, seg[pl.ds(b, 1), :].astype(F32), first, own)
            ctx = mm(probs.astype(BF), qkv[b, :, 2 * HEAD_DIM:]).astype(BF)
            gst[t % 2, d] = mm(ctx, wo[...]).astype(BF).reshape(2, SUB, ROWS, width)
            swap(d, t).start()

    def rs_step(t, first):
        for d in range(2):
            swap(d, t).wait_recv()
        for j in range(SUB):
            for d in range(2):
                m = chunk_at(d, t)
                v = gst[t % 2, d, core, j].astype(F32) + oth[m, d, j].astype(F32)
                if not first:
                    rs_copy(d, j, t - 2, m, rs_sem, rr_sem).wait_recv()
                    v = v + arr[t - 2, d, j].astype(F32)
                loc[m, d, j] = v.astype(BF)
                rs_copy(d, j, t - 1, m, rs_sem, rr_sem).start()

    attend(jnp.int32(1))

    @pl.loop(1, chips)
    def _(t):
        @pl.when(t > 1)
        def _():
            for d in range(2):
                swap(d, t - 1).wait_send()

        attend(t + 1)

        @pl.when(t == 1)
        def _():
            rs_step(t, True)

        @pl.when(t > 1)
        def _():
            rs_step(t, False)

    def ag_copy(d, j, t, m):
        return remote(gat.at[m * 2 + core, d, j], gat.at[m * 2 + core, d, j], as_sem, ar_sem.at[t, d, j], nxt[d])

    def spread(d, j, t, m):
        remote(gat.at[m * 2 + core, d, j], gat.at[m * 2 + core, d, j], ps_sem, pm_sem.at[t], mate).start()

    x_load.wait()
    dy_load.wait()
    for d in range(2):
        swap(d, chips).wait_recv()
    for j in range(SUB):
        for d in range(2):
            rs_copy(d, j, last - 1, chip, rs_sem, rr_sem).wait_recv()
            v = gst[chips % 2, d, core, j].astype(F32) + oth[chip, d, j].astype(F32) + arr[last - 1, d, j].astype(F32)
            h = (x_own[d, j].astype(F32) + v.astype(BF).astype(F32)).astype(BF)
            h_own[d, j] = h
            normed, _ = rms_parts(h)
            gat[me, d, j] = (normed * g_ref[...]).astype(BF)
            ag_copy(d, j, 0, chip).start()
            spread(d, j, 0, chip)

    def bulk(ref, sem, rsem):
        return remote(ref, ref, sem, rsem, mate)

    bulk(arr, rs_sem, pr2_sem).wait_send()
    for t in (chips - 1, chips):
        for d in range(2):
            swap(d, t).wait_send()

    def p_copy(d, t):
        m = chunk_at(d, t)
        return pltpu.make_async_copy(pst.at[t % 2, d], p_out.at[pl.ds(m * 2, 2), d], po_sem.at[t % 2, d])

    def swap2(d, t):
        m = chunk_at(d, t)
        return remote(gst.at[t % 2, d, 1 - core], oth.at[m, d], xs2_sem.at[t % 2, d], xr2_sem.at[m, d], mate)

    def rs2_step(t, first):
        slot = t % 2
        for d in range(2):
            swap2(d, t).wait_recv()
        for j in range(SUB):
            for d in range(2):
                m = chunk_at(d, t)
                v = gst[slot, d, core, j].astype(F32) + oth[m, d, j].astype(F32)
                if not first:
                    rs_copy(d, j, t - 2, m, rs2_sem, rr2_sem).wait_recv()
                    v = v + arr[t - 2, d, j].astype(F32)
                loc[m, d, j] = v.astype(BF)
                rs_copy(d, j, t - 1, m, rs2_sem, rr2_sem).start()

    def collect(t, onward):
        for j in range(SUB):
            for d in range(2):
                m = chunk_at(d, t)
                ag_copy(d, j, t - 1, m).wait_recv()
                if onward:
                    ag_copy(d, j, t, m).start()
                spread(d, j, t, m)

    step = width // 4

    @pl.loop(0, chips)
    def _(t):
        slot = t % 2
        a = chunk_at(0, t)
        b = chunk_at(1, t)

        @pl.when((t > 0) & (t < last))
        def _():
            collect(t, True)

        @pl.when(t == last)
        def _():
            collect(t, False)

        @pl.when(t < last)
        def _():
            for d in range(2):
                dy_copy(d, t + 1).start()

        @pl.when(t >= 2)
        def _():
            for d in range(2):
                p_copy(d, t - 2).wait()
                swap2(d, t - 2).wait_send()

        for d in range(2):
            dy_copy(d, t).wait()
        bulk(gat.at[0], ps_sem, pm_sem.at[t]).wait_recv()

        rows = 4 * SUB * ROWS
        mb = jnp.concatenate([gat[pl.ds(a * 2, 2), 0].reshape(rows // 2, width), gat[pl.ds(b * 2, 2), 1].reshape(rows // 2, width)], axis=0)
        dyv = dyb[slot].reshape(rows, width)
        gate = mm_nt(mb, wg[...])
        upper = mm_nt(mb, wu[...])
        dact = mm_nt(dyv, wd[...])
        sig = jax.nn.sigmoid(gate)
        act = (gate * sig * upper).astype(BF)
        dgate = (dact * upper * sig * (1.0 + gate * (1.0 - sig))).astype(BF)
        dupper = (dact * gate * sig).astype(BF)
        for n in range(4):
            cs = slice(n * step, (n + 1) * step)
            gst[slot, :, :, :, :, cs] = (mm(dgate, wg[:, cs]) + mm(dupper, wu[:, cs])).astype(BF).reshape(2, 2, SUB, ROWS, step)
        for d in range(2):
            swap2(d, t).start()
        for n in range(4):
            cs = slice(n * step, (n + 1) * step)
            pst[slot, :, :, :, :, cs] = mm(act, wd[:, cs]).astype(BF).reshape(2, 2, SUB, ROWS, step)
            dwd[:, cs] += mm_tn(act, dyv[:, cs])
            dwg[:, cs] += mm_tn(dgate, mb[:, cs])
            dwu[:, cs] += mm_tn(dupper, mb[:, cs])
        for d in range(2):
            p_copy(d, t).start()

        @pl.when(t == 0)
        def _():
            for d in range(2):
                loc[chip, d] = gst[0, d, core]

        @pl.when(t == 1)
        def _():
            rs2_step(t, True)

        @pl.when(t > 1)
        def _():
            rs2_step(t, False)

    def ag2_copy(d, j, t, m):
        return remote(gat2.at[m, d, j], gat2.at[m, d, j], as2_sem, ar2_sem.at[t, d, j], nxt[d])

    def spread2(d, j, m):
        remote(gat2.at[m, d, j], out.at[m * 2 + core, d, j], ps2_sem, pr2_sem, mate).start()
        pltpu.make_async_copy(gat2.at[m, d, j], out.at[m * 2 + core, d, j], wo_sem).start()

    for d in range(2):
        swap2(d, 0).wait_recv()
    total = jnp.zeros((1, width), F32)
    for j in range(SUB):
        for d in range(2):
            rs_copy(d, j, last - 1, chip, rs2_sem, rr2_sem).wait_recv()
            v = loc[chip, d, j].astype(F32) + oth[chip, d, j].astype(F32) + arr[last - 1, d, j].astype(F32)
            v = v.astype(BF).astype(F32)
            normed, inv = rms_parts(h_own[d, j])
            total = total + jnp.sum(v * normed, axis=0, keepdims=True)
            grad = dy_own[d, j].astype(F32) + rms_back(v, normed, inv, g_ref[...])
            dres_own[d, j] = grad
            gat2[chip, d, j] = grad.astype(BF)
            ag2_copy(d, j, 0, chip).start()
            spread2(d, j, chip)
    gpart[...] = total

    def ag2_step(t, onward):
        for j in range(SUB):
            for d in range(2):
                m = chunk_at(d, t)
                ag2_copy(d, j, t - 1, m).wait_recv()
                if onward:
                    ag2_copy(d, j, t, m).start()
                spread2(d, j, m)

    @pl.loop(1, last)
    def _(t):
        ag2_step(t, True)

    ag2_step(last, False)

    bulk(gat2, ps2_sem, pr2_sem).wait_recv()
    for sem in (ps_sem, ps2_sem):
        bulk(oth, sem, pr2_sem).wait_send()
    for sem in (as_sem, rs2_sem, as2_sem):
        bulk(arr, sem, pr2_sem).wait_send()
    for t in (chips - 2, chips - 1):
        for d in range(2):
            p_copy(d, t).wait()
            swap2(d, t).wait_send()
    pltpu.make_async_copy(gat2, gat2, wo_sem).wait()


def mid_call(x, dy, gain, seg, qkv, w_o, w_gate, w_up, w_down, chips, cid):
    nb, seq, width = x.shape
    tokens = nb * seq
    ff = w_down.shape[0]
    shape = (chips * 2, 2, SUB, ROWS, width)
    half = (chips, 2, SUB, ROWS, width)
    arrive = (chips - 1, 2, SUB, ROWS, width)
    piece = (2, SUB, ROWS, width)
    pair = (2, 2, 2, SUB, ROWS, width)
    vm = pl.BlockSpec(memory_space=pltpu.VMEM)
    anyspec = pl.BlockSpec(memory_space=pl.ANY)
    dma = pltpu.SemaphoreType.DMA
    steps = dma((chips - 1, 2, SUB))
    vmb = lambda shp: pltpu.VMEM(shp, BF)
    grad = jax.ShapeDtypeStruct((ff, width), F32)
    res = pl.pallas_call(
        functools.partial(mid_kernel, chips),
        out_shape=[jax.ShapeDtypeStruct(shape, BF), jax.ShapeDtypeStruct(shape, BF), jax.ShapeDtypeStruct(piece, BF),
                   jax.ShapeDtypeStruct(piece, BF), jax.ShapeDtypeStruct(piece, F32), jax.ShapeDtypeStruct((1, width), F32),
                   grad, grad, grad],
        in_specs=[anyspec] * 2 + [vm] * 7,
        out_specs=[anyspec] * 2 + [vm] * 7,
        scratch_shapes=[
            vmb(half), vmb(half), vmb(arrive), vmb(shape), vmb(half), vmb(pair), vmb(pair), vmb(pair), vmb(piece),
            dma((2, 2)), dma((chips, 2)), dma, steps, dma, steps, dma, dma((chips,)), dma((2,)), dma((2, 2)), dma((2, 2)),
            dma((2, 2)), dma((chips, 2)), dma, steps, dma, steps, dma, dma, dma],
        name='middle',
        compiler_params=pltpu.CompilerParams(collective_id=cid, has_side_effects=True, vmem_limit_bytes=67_000_000),
        cost_estimate=pl.CostEstimate(flops=120_000_000_000, bytes_accessed=40 * tokens * width, transcendentals=0),
    )(x.reshape(shape), dy.reshape(shape), gain, seg, qkv, w_o, w_gate, w_up, w_down)
    return (res[0].reshape(tokens, width), res[1].reshape(tokens, width)) + tuple(res[2:])


def solution(mesh):
    tp_size = mesh.shape['tp']
    chips = tp_size // 2

    def device_step(hidden, seg_ids, grad_out, gain_attn, gain_mlp, w_q, w_k, w_v, w_o, w_gate, w_up, w_down):
        nb, seq, width = hidden.shape
        tokens = nb * seq
        own = tokens // tp_size
        g1 = gain_attn[None, :]
        g2 = gain_mlp[None, :]
        qkv = front_call(hidden.reshape(tokens, width), g1, w_q, w_k, w_v).reshape(nb, seq, 3 * HEAD_DIM)
        dres, p_part, h_own, x_own, dres_own, g2_part, d_gate, d_up, d_down = mid_call(
            hidden, grad_out, g2, seg_ids, qkv, w_o, w_gate.T, w_up.T, w_down, chips, 1)
        grad_q = jax.ShapeDtypeStruct((width, HEAD_DIM), F32)
        grad_kv = jax.ShapeDtypeStruct((width, 2 * HEAD_DIM), F32)
        grad_o = jax.ShapeDtypeStruct((HEAD_DIM, width), F32)
        y_out, ga_part, d_q, d_kv, d_o = ring_call(
            p_part, [h_own, dres.reshape(nb, seq, width), hidden, seg_ids, g1, w_q, w_k, w_v, w_o, qkv],
            [jax.ShapeDtypeStruct((nb, seq, width), BF), grad_q, grad_kv, grad_o], AddTail, chips, 4,
            task=back_task, in_any=(1, 2), out_any=(0,), extra=back_scratch(seq, width))
        kv_shape = (tp_size, 2, own // 2, 2 * HEAD_DIM)
        dx, gains, d_kv = ring_call(ga_part.reshape(tokens, width), [x_own, dres_own, g1, g1, g2_part, d_kv.reshape(kv_shape)],
                                    [jax.ShapeDtypeStruct((2, width), F32), jax.ShapeDtypeStruct(kv_shape, F32)], AttnTail, chips, 3, True)
        y_out, dx, d_q, d_gate, d_up, d_down, d_o, d_k, d_v, d_g2, d_g1 = finish_call(
            [y_out, dx, d_q], [d_gate, d_up, d_down, d_o], d_kv.reshape(width, 2 * HEAD_DIM), gains)
        return (y_out.reshape(nb, seq, width), dx.reshape(nb, seq, width), d_g1[0], d_g2[0], d_q, d_k, d_v,
                d_o, d_gate.T, d_up.T, d_down)

    spec_act = P('data', None, None)
    spec_rows = P('data', None)
    spec_gain = P(None)
    spec_cols = P(None, 'tp')
    spec_tprows = P('tp', None)
    spec_whole = P(None, None)
    spec_stack = P(('data', 'tp'), None)
    in_specs = (spec_act, spec_rows, spec_act, spec_gain, spec_gain, spec_cols, spec_whole, spec_whole, spec_tprows, spec_cols, spec_cols, spec_tprows)
    out_specs = (spec_act, spec_act, P('data'), P('data'), P('data', 'tp'), spec_rows, spec_rows, spec_stack, P('data', 'tp'), P('data', 'tp'), spec_stack)
    return jax.shard_map(device_step, mesh=mesh, in_specs=in_specs, out_specs=out_specs, check_vma=False)
```

```python
import functools
import jax
import jax.numpy as jnp
from jax import lax
from jax.experimental import pallas as pl
from jax.experimental.pallas import tpu as pltpu
from jax.sharding import PartitionSpec as P

HEAD_DIM = 128
EPS = 1e-5
SUB = 4
ROWS = 16
BLK = 256
BOTH = (0, 1)
BF = jnp.bfloat16
F32 = jnp.float32
MESH = pl.DeviceIdType.MESH
VMEM_LIMIT = 60 * 1024 * 1024


def mm(a, b):
    return lax.dot_general(a, b, (((1,), (0,)), ((), ())), preferred_element_type=F32)


def mm_nt(a, b):
    return lax.dot_general(a, b, (((1,), (1,)), ((), ())), preferred_element_type=F32)


def mm_tn(a, b):
    return lax.dot_general(a, b, (((0,), (0,)), ((), ())), preferred_element_type=F32)


def rms_parts(x_in):
    x_float = x_in.astype(F32)
    inv = lax.rsqrt(jnp.mean(x_float * x_float, axis=-1, keepdims=True) + EPS)
    return x_float * inv, inv


def rms_back(grad, normed, inv, gain):
    scaled = grad * gain
    return inv * (scaled - normed * jnp.mean(scaled * normed, axis=-1, keepdims=True))


def ring_kernel(chips, n_in, n_out, epilogue, with_gain, task, part, *refs):
    ins = refs[:n_in]
    out = refs[n_in]
    outs = refs[n_in + 1:n_in + 1 + n_out]
    scratch = refs[n_in + 1 + n_out:]
    (loc, oth, arr, gat, ld_sem, xs_sem, xr_sem, rs_sem, rr_sem, as_sem, ar_sem, ps_sem, pr_sem, wo_sem) = scratch[:14]
    me = lax.axis_index('tp')
    chip = me // 2
    core = me % 2
    mate = chip * 2 + 1 - core
    nxt = (lax.rem(chip + 1, chips) * 2 + core, lax.rem(chip + chips - 1, chips) * 2 + core)

    def dev(t):
        return {'tp': t}

    barrier = pltpu.get_barrier_semaphore()
    for t in (nxt[0], nxt[1], mate):
        pl.semaphore_signal(barrier, inc=1, device_id=dev(t), device_id_type=MESH)
    pl.semaphore_wait(barrier, 3)

    def chunk_at(d, s):
        off = s if d == 1 else chips - s
        return lax.rem(chip + off, chips)

    def swap(d, s):
        m = chunk_at(d, s)
        return pltpu.make_async_remote_copy(
            src_ref=part.at[m * 2 + 1 - core, d], dst_ref=oth.at[m, d], send_sem=xs_sem,
            recv_sem=xr_sem.at[m, d], device_id=dev(mate), device_id_type=MESH)

    def load(d, s):
        m = chunk_at(d, s)
        return pltpu.make_async_copy(part.at[m * 2 + core, d], loc.at[m, d], ld_sem.at[m, d])

    if with_gain:
        (gacc, gbuf, gmate, gs_sem, gr_sem, gms_sem, gmr_sem, kacc, koth, karr, kxs, kxr, krs, krr, kas, kar, kps, kpr) = scratch[14:]
        kin, kout = ins[5], outs[1]

        def kswap(d, s):
            m = chunk_at(d, s)
            return pltpu.make_async_remote_copy(
                src_ref=kin.at[m * 2 + 1 - core, d], dst_ref=koth.at[m, d], send_sem=kxs,
                recv_sem=kxr.at[m, d], device_id=dev(mate), device_id_type=MESH)

        def krs_copy(d, s, m):
            return pltpu.make_async_remote_copy(
                src_ref=kacc.at[m, d], dst_ref=karr.at[s, d], send_sem=krs,
                recv_sem=krr.at[s, d], device_id=dev(nxt[d]), device_id_type=MESH)

        def kag_copy(d, t, m):
            return pltpu.make_async_remote_copy(
                src_ref=kout.at[m * 2 + core, d], dst_ref=kout.at[m * 2 + core, d], send_sem=kas,
                recv_sem=kar.at[t, d], device_id=dev(nxt[d]), device_id_type=MESH)

        def kspread(d, m):
            pltpu.make_async_remote_copy(
                src_ref=kout.at[m * 2 + core, d], dst_ref=kout.at[m * 2 + core, d], send_sem=kps,
                recv_sem=kpr, device_id=dev(mate), device_id_type=MESH).start()

    for s in range(1, chips + 1):
        for d in BOTH:
            swap(d, s % chips).start()
            load(d, s % chips).start()
            if with_gain:
                kswap(d, s % chips).start()

    def rs_copy(d, j, s, m):
        return pltpu.make_async_remote_copy(
            src_ref=loc.at[m, d, j], dst_ref=arr.at[s, d, j], send_sem=rs_sem,
            recv_sem=rr_sem.at[s, d, j], device_id=dev(nxt[d]), device_id_type=MESH)

    def ready(d, s):
        load(d, s).wait()
        swap(d, s).wait_recv()

    def rs_step(s, first):
        for d in BOTH:
            ready(d, s + 1)
        for j in range(SUB):
            for d in BOTH:
                m = chunk_at(d, s + 1)
                v = loc[m, d, j].astype(F32) + oth[m, d, j].astype(F32)
                if not first:
                    rs_copy(d, j, s - 1, m).wait_recv()
                    v = v + arr[s - 1, d, j].astype(F32)
                loc[m, d, j] = v.astype(BF)
                rs_copy(d, j, s, m).start()
        if with_gain:
            for d in BOTH:
                m = chunk_at(d, s + 1)
                kswap(d, s + 1).wait_recv()
                kv = kin[m * 2 + core, d] + koth[m, d]
                if not first:
                    krs_copy(d, s - 1, m).wait_recv()
                    kv = kv + karr[s - 1, d]
                kacc[m, d] = kv
                krs_copy(d, s, m).start()

    rs_step(0, True)

    if task:
        work, work_end, work_count = task(ins, outs, scratch[14:])

    def work_share(n):
        if task:
            lead = 2 * (2 * chips - 2) - work_count
            if isinstance(n, int):
                work(jnp.int32(n))
            else:
                lo = jnp.where(n < lead, n, 2 * n - lead)
                pl.loop(lo, lo + jnp.where(n < lead, 1, 2))(work)

    work_share(0)

    @pl.loop(1, chips - 1)
    def _(s):
        rs_step(s, False)
        work_share(s)

    def ag_copy(d, j, t, m):
        return pltpu.make_async_remote_copy(
            src_ref=gat.at[m, d, j], dst_ref=gat.at[m, d, j], send_sem=as_sem,
            recv_sem=ar_sem.at[t, d, j], device_id=dev(nxt[d]), device_id_type=MESH)

    def spread(d, j, m):
        pltpu.make_async_remote_copy(
            src_ref=gat.at[m, d, j], dst_ref=out.at[m * 2 + core, d, j], send_sem=ps_sem,
            recv_sem=pr_sem, device_id=dev(mate), device_id_type=MESH).start()
        pltpu.make_async_copy(gat.at[m, d, j], out.at[m * 2 + core, d, j], wo_sem).start()

    for d in BOTH:
        ready(d, 0)
    state = epilogue.begin(ins, outs)
    for j in range(SUB):
        for d in BOTH:
            rs_copy(d, j, chips - 2, chip).wait_recv()
            v = loc[chip, d, j].astype(F32) + oth[chip, d, j].astype(F32) + arr[chips - 2, d, j].astype(F32)
            res, state = epilogue.piece(v.astype(BF).astype(F32), d, j, ins, outs, state)
            gat[chip, d, j] = res
            ag_copy(d, j, 0, chip).start()
            spread(d, j, chip)
    epilogue.end(outs, state)

    work_share(chips - 1)

    if with_gain:
        for d in BOTH:
            kswap(d, 0).wait_recv()
            krs_copy(d, chips - 2, chip).wait_recv()
            kout[chip * 2 + core, d] = kin[chip * 2 + core, d] + koth[chip, d] + karr[chips - 2, d]
            kag_copy(d, 0, chip).start()
            kspread(d, chip)

        def gain_copy(t, src):
            return pltpu.make_async_remote_copy(
                src_ref=src, dst_ref=gbuf.at[t], send_sem=gs_sem.at[t],
                recv_sem=gr_sem.at[t], device_id=dev(nxt[0]), device_id_type=MESH)

        gacc[0:1] = ins[4][...]
        gacc[1:2] = state
        gain_copy(0, gacc).start()

    def ag_step(t, last):
        for j in range(SUB):
            for d in BOTH:
                m = chunk_at(d, t)
                ag_copy(d, j, t - 1, m).wait_recv()
                if not last:
                    ag_copy(d, j, t, m).start()
                spread(d, j, m)
        if with_gain:
            for d in BOTH:
                m = chunk_at(d, t)
                kag_copy(d, t - 1, m).wait_recv()
                if not last:
                    kag_copy(d, t, m).start()
                kspread(d, m)
            gain_copy(t - 1, gacc).wait_recv()
            if not last:
                gain_copy(t, gbuf.at[t - 1]).start()

    @pl.loop(1, chips - 1)
    def _(t):
        ag_step(t, False)
        work_share(chips - 1 + t)

    ag_step(chips - 1, True)
    if task:
        work_end()

    if with_gain:
        tot = gacc[...]
        for t in range(chips - 1):
            tot = tot + gbuf[t]
            gain_copy(t, gacc).wait_send()
        outs[0][...] = tot
        mate_copy = pltpu.make_async_remote_copy(
            src_ref=outs[0], dst_ref=gmate, send_sem=gms_sem, recv_sem=gmr_sem,
            device_id=dev(mate), device_id_type=MESH)
        mate_copy.start()
        mate_copy.wait()
        outs[0][...] = tot + gmate[...]

    def bulk(ref, sem, rsem):
        return pltpu.make_async_remote_copy(
            src_ref=ref, dst_ref=ref, send_sem=sem, recv_sem=rsem, device_id=dev(mate), device_id_type=MESH)

    if with_gain:
        bulk(koth, kps, kpr).wait_recv()
        bulk(koth, kxs, kpr).wait_send()
        bulk(karr, krs, kpr).wait_send()
        bulk(karr, kas, kpr).wait_send()
        bulk(koth, kps, kpr).wait_send()
    bulk(gat, ps_sem, pr_sem).wait_recv()
    bulk(oth, xs_sem, pr_sem).wait_send()
    bulk(arr, rs_sem, pr_sem).wait_send()
    bulk(arr, as_sem, pr_sem).wait_send()
    bulk(gat, ps_sem, pr_sem).wait_send()
    pltpu.make_async_copy(gat, gat, wo_sem).wait()


class AddTail:
    @staticmethod
    def begin(ins, outs):
        return None

    @staticmethod
    def piece(v, d, j, ins, outs, state):
        return (ins[0][d, j].astype(F32) + v).astype(BF), state

    @staticmethod
    def end(outs, state):
        pass


class AttnTail:
    @staticmethod
    def begin(ins, outs):
        return jnp.zeros(ins[2].shape, F32)

    @staticmethod
    def piece(v, d, j, ins, outs, state):
        normed, inv = rms_parts(ins[0][d, j])
        state = state + jnp.sum(v * normed, axis=0, keepdims=True)
        grad = ins[1][d, j] + rms_back(v, normed, inv, ins[2][...])
        return grad.astype(BF), state

    @staticmethod
    def end(outs, state):
        pass


def ring_call(part, ins, out_shapes, epilogue, chips, cid, with_gain=False, task=None, in_any=(), out_any=(), extra=()):
    tokens, width = part.shape
    shape = (chips * 2, 2, SUB, ROWS, width)
    half = (chips, 2, SUB, ROWS, width)
    arrive = (chips - 1, 2, SUB, ROWS, width)
    vm = pl.BlockSpec(memory_space=pltpu.VMEM)
    anyspec = pl.BlockSpec(memory_space=pl.ANY)
    dma = pltpu.SemaphoreType.DMA
    scratch = [
        pltpu.VMEM(half, BF), pltpu.VMEM(half, BF), pltpu.VMEM(arrive, BF), pltpu.VMEM(half, BF),
        dma((chips, 2)), dma, dma((chips, 2)), dma, dma((chips - 1, 2, SUB)), dma,
        dma((chips - 1, 2, SUB)), dma, dma, dma]
    if with_gain:
        scratch += [pltpu.VMEM((2, width), F32), pltpu.VMEM((chips - 1, 2, width), F32), pltpu.VMEM((2, width), F32),
                    dma((chips - 1,)), dma((chips - 1,)), dma, dma]
        kshape = ins[5].shape[1:]
        scratch += [pltpu.VMEM((chips,) + kshape, F32), pltpu.VMEM((chips,) + kshape, F32), pltpu.VMEM((chips - 1,) + kshape, F32),
                    dma, dma((chips, 2)), dma, dma((chips - 1, 2)), dma, dma((chips - 1, 2)), dma, dma]
    scratch += list(extra)
    n_in, n_out = len(ins), len(out_shapes)

    def body(*refs):
        ring_kernel(chips, n_in, n_out, epilogue, with_gain, task, *refs)

    res = pl.pallas_call(
        body,
        out_shape=[jax.ShapeDtypeStruct(shape, BF)] + out_shapes,
        in_specs=[anyspec] + [anyspec if n in in_any else vm for n in range(n_in)],
        out_specs=[anyspec] + [anyspec if n in out_any else vm for n in range(n_out)],
        scratch_shapes=scratch,
        name='ring_%d' % cid,
        compiler_params=pltpu.CompilerParams(collective_id=cid, has_side_effects=True, vmem_limit_bytes=VMEM_LIMIT),
        cost_estimate=pl.CostEstimate(flops=80_000_000_000, bytes_accessed=4 * tokens * width, transcendentals=0),
    )(part.reshape(shape), *ins)
    return (res[0].reshape(tokens, width),) + tuple(res[1:])


def seg_column(seg_ref, b, row0, n):
    own = seg_ref[pl.ds(b, 1), pl.ds(row0, n)].astype(F32)
    return jnp.transpose(jnp.broadcast_to(own, (128, n)))[:, :1]


def masked_probs(q, k, seg_q, seg_k, row0, split=0):
    s = mm_nt(q, k) * HEAD_DIM ** -0.5
    local = lax.broadcasted_iota(jnp.int32, s.shape, 0)
    rows = row0 + local
    if split:
        rows = rows + jnp.where(local >= q.shape[0] // 2, split, 0)
    cols = lax.broadcasted_iota(jnp.int32, s.shape, 1)
    s = jnp.where((rows >= cols) & (seg_q == seg_k), s, -1e30)
    e = jnp.exp(s - jnp.max(s, axis=-1, keepdims=True))
    return e * (1.0 / jnp.sum(e, axis=-1, keepdims=True))


def pack(w_ref, wq_ref, wk_ref, wv_ref):
    for n, ref in enumerate((wq_ref, wk_ref, wv_ref)):
        w_ref[:, n * HEAD_DIM:(n + 1) * HEAD_DIM] = ref[...]


def front_kernel(x_ref, g_ref, wq_ref, wk_ref, wv_ref, qkv_ref, w_ref):
    @pl.when(pl.program_id(0) == 0)
    def _():
        pack(w_ref, wq_ref, wk_ref, wv_ref)

    normed, _ = rms_parts(x_ref[...])
    qkv_ref[...] = mm((normed * g_ref[...]).astype(BF), w_ref[...]).astype(BF)


def front_call(x, gain, w_q, w_k, w_v):
    tokens, width = x.shape
    e3 = 3 * HEAD_DIM
    rowblk = lambda n: pl.BlockSpec((BLK, n), lambda i: (i, 0))
    whole = lambda arr: pl.BlockSpec(arr.shape, lambda i: (0, 0))
    return pl.pallas_call(
        front_kernel,
        grid=(tokens // BLK,),
        in_specs=[rowblk(width), whole(gain), whole(w_q), whole(w_k), whole(w_v)],
        out_specs=rowblk(e3),
        out_shape=jax.ShapeDtypeStruct((tokens, e3), BF),
        scratch_shapes=[pltpu.VMEM((width, e3), BF)],
        name='front',
        compiler_params=pltpu.CompilerParams(vmem_limit_bytes=VMEM_LIMIT),
        cost_estimate=pl.CostEstimate(flops=4_000_000_000, bytes_accessed=12_000_000, transcendentals=0),
    )(x, gain, w_q, w_k, w_v)


def back_task(ins, outs, scratch):
    dr_ref, x_ref, sg_ref, g_ref, wq_ref, wk_ref, wv_ref, wo_ref, qkv_ref = ins[1:]
    ga_ref, dwq_ref, dkv_ref, dwo_ref = outs
    inb, gab, dqkv_s, dk_s, dv_s, w_ref, in_sem, ga_sem = scratch
    nb, seq, width = dr_ref.shape
    nq = seq // BLK
    count = nb * 2 * nq
    scale = HEAD_DIM ** -0.5

    def fetch(n):
        b, ph = n // (2 * nq), n % (2 * nq)
        row0 = pl.multiple_of((ph % nq) * BLK, BLK)

        @pl.when(ph < nq)
        def _():
            pltpu.make_async_copy(dr_ref.at[b, pl.ds(row0, BLK)], inb.at[n % 2], in_sem.at[n % 2]).start()

        @pl.when(ph >= nq)
        def _():
            pltpu.make_async_copy(x_ref.at[b, pl.ds(row0, BLK)], inb.at[n % 2], in_sem.at[n % 2]).start()

    def ga_copy(b, i):
        row0 = pl.multiple_of(i * BLK, BLK)
        return pltpu.make_async_copy(gab.at[i % 2], ga_ref.at[b, pl.ds(row0, BLK)], ga_sem.at[i % 2])

    pltpu.make_async_copy(dr_ref.at[0, pl.ds(0, BLK)], inb.at[0], in_sem.at[0]).start()
    pack(w_ref, wq_ref, wk_ref, wv_ref)
    dwq_ref[...] = jnp.zeros_like(dwq_ref)
    dkv_ref[...] = jnp.zeros_like(dkv_ref)
    dwo_ref[...] = jnp.zeros_like(dwo_ref)

    def work(n):
        b, ph = n // (2 * nq), n % (2 * nq)
        row0 = pl.multiple_of((ph % nq) * BLK, BLK)

        @pl.when(n + 1 < count)
        def _():
            fetch(n + 1)

        pltpu.make_async_copy(dr_ref.at[0, pl.ds(0, BLK)], inb.at[n % 2], in_sem.at[n % 2]).wait()

        @pl.when(ph == 0)
        def _():
            dk_s[...] = jnp.zeros_like(dk_s)
            dv_s[...] = jnp.zeros_like(dv_s)

        @pl.when(ph < nq)
        def _():
            dr = inb[n % 2]
            dctx = mm_nt(dr, wo_ref[...]).astype(BF)
            q = qkv_ref[b, pl.ds(row0, BLK), :HEAD_DIM]
            k = qkv_ref[b, :, HEAD_DIM:2 * HEAD_DIM]
            v = qkv_ref[b, :, 2 * HEAD_DIM:]
            probs = masked_probs(q, k, seg_column(sg_ref, b, row0, BLK), sg_ref[pl.ds(b, 1), :].astype(F32), row0)
            probs_b = probs.astype(BF)
            dwo_ref[...] += mm_tn(mm(probs_b, v).astype(BF), dr)
            dp = mm_nt(dctx, v)
            ds = (probs * (dp - jnp.sum(dp * probs, axis=-1, keepdims=True)) * scale).astype(BF)
            dv_s[...] += mm_tn(probs_b, dctx)
            dk_s[...] += mm_tn(ds, q)
            dqkv_s[pl.ds(row0, BLK), :HEAD_DIM] = mm(ds, k).astype(BF)

        @pl.when(ph == nq - 1)
        def _():
            dqkv_s[:, HEAD_DIM:2 * HEAD_DIM] = dk_s[...].astype(BF)
            dqkv_s[:, 2 * HEAD_DIM:] = dv_s[...].astype(BF)

        @pl.when(ph >= nq)
        def _():
            i = ph - nq
            normed, _ = rms_parts(inb[n % 2])
            a = (normed * g_ref[...]).astype(BF)
            blk = dqkv_s[pl.ds(row0, BLK)]
            dw = mm_tn(a, blk)
            dwq_ref[...] += dw[:, :HEAD_DIM]
            dkv_ref[...] += dw[:, HEAD_DIM:]

            @pl.when((b > 0) | (i >= 2))
            def _():
                ga_copy(b, i).wait()

            gab[i % 2] = mm_nt(blk, w_ref[...]).astype(BF)
            ga_copy(b, i).start()

    def end():
        for i in (nq - 2, nq - 1):
            ga_copy(nb - 1, i).wait()

    return work, end, count


def back_scratch(seq, width):
    return [pltpu.VMEM((2, BLK, width), BF), pltpu.VMEM((2, BLK, width), BF), pltpu.VMEM((seq, 3 * HEAD_DIM), BF),
            pltpu.VMEM((seq, HEAD_DIM), F32), pltpu.VMEM((seq, HEAD_DIM), F32), pltpu.VMEM((width, 3 * HEAD_DIM), BF),
            pltpu.SemaphoreType.DMA((2,)), pltpu.SemaphoreType.DMA((2,))]


def finish_kernel(cuts, *refs):
    n = len(cuts)
    ins, kv, gains = refs[:n], refs[n], refs[n + 1]
    outs, dk, dv, first, second = refs[n + 2:2 * n + 2], refs[2 * n + 2], refs[2 * n + 3], refs[2 * n + 4], refs[2 * n + 5]
    bufs, kv_buf, rd_sem, wr_sem = refs[2 * n + 6:3 * n + 6], refs[3 * n + 6], refs[3 * n + 7], refs[3 * n + 8]
    reads, writes = [], []
    for src, dst, buf, parts in zip(ins, outs, bufs, cuts):
        size = src.shape[0] // parts
        for p in range(parts):
            at = pl.ds(p * size, size)
            reads.append(pltpu.make_async_copy(src.at[at], buf.at[at], rd_sem.at[len(reads)]))
            writes.append([pltpu.make_async_copy(buf.at[at], dst.at[at], wr_sem.at[len(writes)])])
    reads.append(pltpu.make_async_copy(kv, kv_buf, rd_sem.at[len(reads)]))
    base = len(writes)
    writes.append([pltpu.make_async_copy(kv_buf.at[:, pl.ds(k * HEAD_DIM, HEAD_DIM)], dst, wr_sem.at[base + k]) for k, dst in enumerate((dk, dv))])
    for copy in reads:
        copy.start()
    first[...] = gains[0:1, :]
    second[...] = gains[1:2, :]
    for copy, group in zip(reads, writes):
        copy.wait()
        for put in group:
            put.start()
    for group in writes:
        for put in group:
            put.wait()


def finish_call(copied, cuts, kv, gains):
    half = jax.ShapeDtypeStruct((kv.shape[0], HEAD_DIM), F32)
    gain = jax.ShapeDtypeStruct((1, gains.shape[1]), F32)
    vm = pl.BlockSpec(memory_space=pltpu.VMEM)
    anyspec = pl.BlockSpec(memory_space=pl.ANY)
    n = len(copied)
    dma = pltpu.SemaphoreType.DMA
    return pl.pallas_call(
        functools.partial(finish_kernel, cuts),
        in_specs=[anyspec] * (n + 1) + [vm],
        out_specs=[anyspec] * (n + 2) + [vm, vm],
        out_shape=[jax.ShapeDtypeStruct(a.shape, a.dtype) for a in copied] + [half, half, gain, gain],
        scratch_shapes=[pltpu.VMEM(a.shape, a.dtype) for a in copied] + [pltpu.VMEM(kv.shape, F32), dma((sum(cuts) + 1,)), dma((sum(cuts) + 2,))],
        name='finish',
        compiler_params=pltpu.CompilerParams(vmem_limit_bytes=VMEM_LIMIT),
        cost_estimate=pl.CostEstimate(flops=1_000_000_000, bytes_accessed=60_000_000, transcendentals=0),
    )(*copied, kv, gains)


def mid_kernel(chips, x, dy, g_ref, seg, qkv, wo, wg_in, wu_in, wd_in, out, p_out, h_own, x_own, dres_own, gpart, dwg_out, dwu_out, dwd_out,
               loc, oth, arr, gat, gat2, dyb, pst, gst, dy_own, wg, wu, wd, dwg, dwu, dwd, w_sem, dw_sem,
               xs_sem, xr_sem, rs_sem, rr_sem, as_sem, ar_sem, ps_sem, pm_sem, own_sem, dy_sem, po_sem,
               xs2_sem, xr2_sem, rs2_sem, rr2_sem, as2_sem, ar2_sem, ps2_sem, pr2_sem, wo_sem):
    me = lax.axis_index('tp')
    chip = me // 2
    core = me % 2
    mate = chip * 2 + 1 - core
    nxt = (lax.rem(chip + 1, chips) * 2 + core, lax.rem(chip + chips - 1, chips) * 2 + core)
    width = x.shape[-1]
    last = chips - 1

    def remote(src, dst, ssem, rsem, t):
        return pltpu.make_async_remote_copy(src_ref=src, dst_ref=dst, send_sem=ssem, recv_sem=rsem,
                                            device_id={'tp': t}, device_id_type=MESH)

    barrier = pltpu.get_barrier_semaphore()
    for t in (nxt[0], nxt[1], mate):
        pl.semaphore_signal(barrier, inc=1, device_id={'tp': t}, device_id_type=MESH)
    pl.semaphore_wait(barrier, 3)

    def chunk_at(d, s):
        return lax.rem(chip + (s if d == 1 else chips - s), chips)

    def swap(d, t):
        m = chunk_at(d, t)
        return remote(gst.at[t % 2, d, 1 - core], oth.at[m, d], xs_sem.at[t % 2, d], xr_sem.at[m, d], mate)

    def dy_copy(d, t):
        m = chunk_at(d, t)
        return pltpu.make_async_copy(dy.at[pl.ds(m * 2, 2), d], dyb.at[t % 2, d], dy_sem.at[t % 2, d])

    weights = [pltpu.make_async_copy(src, dst, w_sem.at[n]) for n, (src, dst) in enumerate(((wg_in, wg), (wu_in, wu), (wd_in, wd)))]
    grads = [pltpu.make_async_copy(src, dst, dw_sem.at[n]) for n, (src, dst) in enumerate(((dwg, dwg_out), (dwu, dwu_out), (dwd, dwd_out)))]
    for copy in weights:
        copy.start()
    x_load = pltpu.make_async_copy(x.at[me], x_own, own_sem.at[0])
    dy_load = pltpu.make_async_copy(dy.at[me], dy_own, own_sem.at[1])
    x_load.start()
    dy_load.start()
    for d in BOTH:
        dy_copy(d, 0).start()
    for acc in (dwg, dwu, dwd):
        acc[...] = jnp.zeros_like(acc)

    def rs_copy(d, j, s, m, ssem, rsem):
        return remote(loc.at[m, d, j], arr.at[s, d, j], ssem, rsem.at[s, d, j], nxt[d])

    own = SUB * ROWS
    group = chips // qkv.shape[0]

    def attend(t):
        for d in BOTH:
            m = chunk_at(d, t)
            b = m // group
            base = pl.multiple_of((m % group) * 4 * own, 4 * own)
            first = pl.multiple_of(base + d * own, own)
            again = pl.multiple_of(base + (2 + d) * own, own)
            q = jnp.concatenate([qkv[b, pl.ds(first, own), :HEAD_DIM], qkv[b, pl.ds(again, own), :HEAD_DIM]], axis=0)
            col = seg_column(seg, b, base, 4 * own)
            seg_q = jnp.concatenate([col[d * own:(d + 1) * own], col[(2 + d) * own:(3 + d) * own]], axis=0)
            probs = masked_probs(q, qkv[b, :, HEAD_DIM:2 * HEAD_DIM], seg_q, seg[pl.ds(b, 1), :].astype(F32), first, own)
            ctx = mm(probs.astype(BF), qkv[b, :, 2 * HEAD_DIM:]).astype(BF)
            gst[t % 2, d] = mm(ctx, wo[...]).astype(BF).reshape(2, SUB, ROWS, width)
            swap(d, t).start()

    def rs_step(t, first):
        for d in BOTH:
            swap(d, t).wait_recv()
        for j in range(SUB):
            for d in BOTH:
                m = chunk_at(d, t)
                v = gst[t % 2, d, core, j].astype(F32) + oth[m, d, j].astype(F32)
                if not first:
                    rs_copy(d, j, t - 2, m, rs_sem, rr_sem).wait_recv()
                    v = v + arr[t - 2, d, j].astype(F32)
                loc[m, d, j] = v.astype(BF)
                rs_copy(d, j, t - 1, m, rs_sem, rr_sem).start()

    attend(jnp.int32(1))
    rs_step(1, True)
    attend(jnp.int32(2))

    @pl.loop(2, chips)
    def _(t):
        for d in BOTH:
            swap(d, t - 1).wait_send()
        attend(t + 1)
        rs_step(t, False)

    def ag_copy(d, j, t, m):
        return remote(gat.at[m * 2 + core, d, j], gat.at[m * 2 + core, d, j], as_sem, ar_sem.at[t, d, j], nxt[d])

    def spread(d, j, t, m):
        remote(gat.at[m * 2 + core, d, j], gat.at[m * 2 + core, d, j], ps_sem, pm_sem.at[t], mate).start()

    x_load.wait()
    dy_load.wait()
    for d in BOTH:
        swap(d, chips).wait_recv()
    for j in range(SUB):
        for d in BOTH:
            rs_copy(d, j, last - 1, chip, rs_sem, rr_sem).wait_recv()
            v = gst[chips % 2, d, core, j].astype(F32) + oth[chip, d, j].astype(F32) + arr[last - 1, d, j].astype(F32)
            h = (x_own[d, j].astype(F32) + v.astype(BF).astype(F32)).astype(BF)
            h_own[d, j] = h
            normed, _ = rms_parts(h)
            gat[me, d, j] = (normed * g_ref[...]).astype(BF)
            ag_copy(d, j, 0, chip).start()
            spread(d, j, 0, chip)

    def bulk(ref, sem, rsem):
        return remote(ref, ref, sem, rsem, mate)

    bulk(arr, rs_sem, pr2_sem).wait_send()
    for t in (chips - 1, chips):
        for d in BOTH:
            swap(d, t).wait_send()

    def p_copy(d, t):
        m = chunk_at(d, t)
        return pltpu.make_async_copy(pst.at[t % 2, d], p_out.at[pl.ds(m * 2, 2), d], po_sem.at[t % 2, d])

    def swap2(d, t):
        m = chunk_at(d, t)
        return remote(gst.at[t % 2, d, 1 - core], oth.at[m, d], xs2_sem.at[t % 2, d], xr2_sem.at[m, d], mate)

    def rs2_step(t, first):
        slot = t % 2
        for d in BOTH:
            swap2(d, t).wait_recv()
        for j in range(SUB):
            for d in BOTH:
                m = chunk_at(d, t)
                v = gst[slot, d, core, j].astype(F32) + oth[m, d, j].astype(F32)
                if not first:
                    rs_copy(d, j, t - 2, m, rs2_sem, rr2_sem).wait_recv()
                    v = v + arr[t - 2, d, j].astype(F32)
                loc[m, d, j] = v.astype(BF)
                rs_copy(d, j, t - 1, m, rs2_sem, rr2_sem).start()

    def collect(t, onward):
        for j in range(SUB):
            for d in BOTH:
                m = chunk_at(d, t)
                ag_copy(d, j, t - 1, m).wait_recv()
                if onward:
                    ag_copy(d, j, t, m).start()
                spread(d, j, t, m)

    step = width // 4
    for copy in weights:
        copy.wait()

    @pl.loop(0, chips)
    def _(t):
        slot = t % 2
        a = chunk_at(0, t)
        b = chunk_at(1, t)

        @pl.when((t > 0) & (t < last))
        def _():
            collect(t, True)

        @pl.when(t == last)
        def _():
            collect(t, False)

        @pl.when(t < last)
        def _():
            for d in BOTH:
                dy_copy(d, t + 1).start()

        @pl.when(t >= 2)
        def _():
            for d in BOTH:
                p_copy(d, t - 2).wait()
                swap2(d, t - 2).wait_send()

        for d in BOTH:
            dy_copy(d, t).wait()
        bulk(gat.at[0], ps_sem, pm_sem.at[t]).wait_recv()

        rows = 4 * SUB * ROWS
        mb = jnp.concatenate([gat[pl.ds(a * 2, 2), 0].reshape(rows // 2, width), gat[pl.ds(b * 2, 2), 1].reshape(rows // 2, width)], axis=0)
        dyv = dyb[slot].reshape(rows, width)
        gate = mm_nt(mb, wg[...])
        upper = mm_nt(mb, wu[...])
        dact = mm_nt(dyv, wd[...])
        sig = jax.nn.sigmoid(gate)
        act = (gate * sig * upper).astype(BF)
        dgate = (dact * upper * sig * (1.0 + gate * (1.0 - sig))).astype(BF)
        dupper = (dact * gate * sig).astype(BF)
        for n in range(4):
            cs = slice(n * step, (n + 1) * step)
            gst[slot, :, :, :, :, cs] = (mm(dgate, wg[:, cs]) + mm(dupper, wu[:, cs])).astype(BF).reshape(2, 2, SUB, ROWS, step)
        for d in BOTH:
            swap2(d, t).start()
        for n in range(4):
            cs = slice(n * step, (n + 1) * step)
            pst[slot, :, :, :, :, cs] = mm(act, wd[:, cs]).astype(BF).reshape(2, 2, SUB, ROWS, step)
            dwd[:, cs] += mm_tn(act, dyv[:, cs])
            dwg[:, cs] += mm_tn(dgate, mb[:, cs])
            dwu[:, cs] += mm_tn(dupper, mb[:, cs])
        for d in BOTH:
            p_copy(d, t).start()

        @pl.when(t == 0)
        def _():
            for d in BOTH:
                loc[chip, d] = gst[0, d, core]

        @pl.when(t == 1)
        def _():
            rs2_step(t, True)

        @pl.when(t > 1)
        def _():
            rs2_step(t, False)

    for copy in grads:
        copy.start()

    def ag2_copy(d, j, t, m):
        return remote(gat2.at[m, d, j], gat2.at[m, d, j], as2_sem, ar2_sem.at[t, d, j], nxt[d])

    def spread2(d, j, m):
        remote(gat2.at[m, d, j], out.at[m * 2 + core, d, j], ps2_sem, pr2_sem, mate).start()
        pltpu.make_async_copy(gat2.at[m, d, j], out.at[m * 2 + core, d, j], wo_sem).start()

    for d in BOTH:
        swap2(d, 0).wait_recv()
    total = jnp.zeros((1, width), F32)
    for j in range(SUB):
        for d in BOTH:
            rs_copy(d, j, last - 1, chip, rs2_sem, rr2_sem).wait_recv()
            v = loc[chip, d, j].astype(F32) + oth[chip, d, j].astype(F32) + arr[last - 1, d, j].astype(F32)
            v = v.astype(BF).astype(F32)
            normed, inv = rms_parts(h_own[d, j])
            total = total + jnp.sum(v * normed, axis=0, keepdims=True)
            grad = dy_own[d, j].astype(F32) + rms_back(v, normed, inv, g_ref[...])
            dres_own[d, j] = grad
            gat2[chip, d, j] = grad.astype(BF)
            ag2_copy(d, j, 0, chip).start()
            spread2(d, j, chip)
    gpart[...] = total

    def ag2_step(t, onward):
        for j in range(SUB):
            for d in BOTH:
                m = chunk_at(d, t)
                ag2_copy(d, j, t - 1, m).wait_recv()
                if onward:
                    ag2_copy(d, j, t, m).start()
                spread2(d, j, m)

    @pl.loop(1, last)
    def _(t):
        ag2_step(t, True)

    ag2_step(last, False)

    bulk(gat2, ps2_sem, pr2_sem).wait_recv()
    for sem in (ps_sem, ps2_sem):
        bulk(oth, sem, pr2_sem).wait_send()
    for sem in (as_sem, rs2_sem, as2_sem):
        bulk(arr, sem, pr2_sem).wait_send()
    for t in (chips - 2, chips - 1):
        for d in BOTH:
            p_copy(d, t).wait()
            swap2(d, t).wait_send()
    pltpu.make_async_copy(gat2, gat2, wo_sem).wait()
    for copy in grads:
        copy.wait()


def mid_call(x, dy, gain, seg, qkv, w_o, w_gate, w_up, w_down, chips, cid):
    nb, seq, width = x.shape
    tokens = nb * seq
    ff = w_down.shape[0]
    shape = (chips * 2, 2, SUB, ROWS, width)
    half = (chips, 2, SUB, ROWS, width)
    arrive = (chips - 1, 2, SUB, ROWS, width)
    piece = (2, SUB, ROWS, width)
    pair = (2, 2, 2, SUB, ROWS, width)
    vm = pl.BlockSpec(memory_space=pltpu.VMEM)
    anyspec = pl.BlockSpec(memory_space=pl.ANY)
    dma = pltpu.SemaphoreType.DMA
    steps = dma((chips - 1, 2, SUB))
    vmb = lambda shp: pltpu.VMEM(shp, BF)
    grad = jax.ShapeDtypeStruct((ff, width), F32)
    weight, acc = vmb((ff, width)), pltpu.VMEM((ff, width), F32)
    res = pl.pallas_call(
        functools.partial(mid_kernel, chips),
        out_shape=[jax.ShapeDtypeStruct(shape, BF), jax.ShapeDtypeStruct(shape, BF), jax.ShapeDtypeStruct(piece, BF),
                   jax.ShapeDtypeStruct(piece, BF), jax.ShapeDtypeStruct(piece, F32), jax.ShapeDtypeStruct((1, width), F32),
                   grad, grad, grad],
        in_specs=[anyspec, anyspec] + [vm] * 4 + [anyspec] * 3,
        out_specs=[anyspec, anyspec] + [vm] * 4 + [anyspec] * 3,
        scratch_shapes=[
            vmb(half), vmb(half), vmb(arrive), vmb(shape), vmb(half), vmb(pair), vmb(pair), vmb(pair), vmb(piece),
            weight, weight, weight, acc, acc, acc, dma((3,)), dma((3,)),
            dma((2, 2)), dma((chips, 2)), dma, steps, dma, steps, dma, dma((chips,)), dma((2,)), dma((2, 2)), dma((2, 2)),
            dma((2, 2)), dma((chips, 2)), dma, steps, dma, steps, dma, dma, dma],
        name='middle',
        compiler_params=pltpu.CompilerParams(collective_id=cid, has_side_effects=True, vmem_limit_bytes=67_000_000),
        cost_estimate=pl.CostEstimate(flops=120_000_000_000, bytes_accessed=40 * tokens * width, transcendentals=0),
    )(x.reshape(shape), dy.reshape(shape), gain, seg, qkv, w_o, w_gate, w_up, w_down)
    return (res[0].reshape(tokens, width), res[1].reshape(tokens, width)) + tuple(res[2:])


def solution(mesh):
    tp_size = mesh.shape['tp']
    chips = tp_size // 2

    def device_step(hidden, seg_ids, grad_out, gain_attn, gain_mlp, w_q, w_k, w_v, w_o, w_gate, w_up, w_down):
        nb, seq, width = hidden.shape
        tokens = nb * seq
        own = tokens // tp_size
        g1 = gain_attn[None, :]
        g2 = gain_mlp[None, :]
        qkv = front_call(hidden.reshape(tokens, width), g1, w_q, w_k, w_v).reshape(nb, seq, 3 * HEAD_DIM)
        dres, p_part, h_own, x_own, dres_own, g2_part, d_gate, d_up, d_down = mid_call(
            hidden, grad_out, g2, seg_ids, qkv, w_o, w_gate.T, w_up.T, w_down, chips, 1)
        grad_q = jax.ShapeDtypeStruct((width, HEAD_DIM), F32)
        grad_kv = jax.ShapeDtypeStruct((width, 2 * HEAD_DIM), F32)
        grad_o = jax.ShapeDtypeStruct((HEAD_DIM, width), F32)
        y_out, ga_part, d_q, d_kv, d_o = ring_call(
            p_part, [h_own, dres.reshape(nb, seq, width), hidden, seg_ids, g1, w_q, w_k, w_v, w_o, qkv],
            [jax.ShapeDtypeStruct((nb, seq, width), BF), grad_q, grad_kv, grad_o], AddTail, chips, 4,
            task=back_task, in_any=(1, 2), out_any=(0,), extra=back_scratch(seq, width))
        kv_shape = (tp_size, 2, own // 2, 2 * HEAD_DIM)
        dx, gains, d_kv = ring_call(ga_part.reshape(tokens, width), [x_own, dres_own, g1, g1, g2_part, d_kv.reshape(kv_shape)],
                                    [jax.ShapeDtypeStruct((2, width), F32), jax.ShapeDtypeStruct(kv_shape, F32)], AttnTail, chips, 3, True)
        y_out, dx, d_q, d_gate, d_up, d_down, d_o, d_k, d_v, d_g2, d_g1 = finish_call(
            [y_out, dx, d_q, d_gate, d_up, d_down, d_o], (4, 4, 1, 2, 2, 2, 1), d_kv.reshape(width, 2 * HEAD_DIM), gains)
        return (y_out.reshape(nb, seq, width), dx.reshape(nb, seq, width), d_g1[0], d_g2[0], d_q, d_k, d_v,
                d_o, d_gate.T, d_up.T, d_down)

    spec_act = P('data', None, None)
    spec_rows = P('data', None)
    spec_gain = P(None)
    spec_cols = P(None, 'tp')
    spec_tprows = P('tp', None)
    spec_whole = P(None, None)
    spec_stack = P(('data', 'tp'), None)
    in_specs = (spec_act, spec_rows, spec_act, spec_gain, spec_gain, spec_cols, spec_whole, spec_whole, spec_tprows, spec_cols, spec_cols, spec_tprows)
    out_specs = (spec_act, spec_act, P('data'), P('data'), P('data', 'tp'), spec_rows, spec_rows, spec_stack, P('data', 'tp'), P('data', 'tp'), spec_stack)
    return jax.shard_map(device_step, mesh=mesh, in_specs=in_specs, out_specs=out_specs, check_vma=False)
```
